32 devices in a mesh: groups: 2 (over y), geom: 4 (over z), design: 2 (over x), head: 2 (over core).
Axes of the slice: x: 2, y: 2, z: 4, core: 2. Of those that a mesh axis runs over, the one named last changes fastest.
Arguments:
- point_feats: bfloat16 [4, 12288, 192], P(('groups', 'design'), ('geom', 'head')), parts along dimension 0, may hold values from -6 to 6
- block_anchor: int32 [4, 96], P(('groups', 'design'), ('geom', 'head')), parts along dimension 0, may hold values from 0 to 127, as said below
- anchor_feats: bfloat16 [4, 128, 192], P(('groups', 'design'), ('geom', 'head')), parts along dimension 0, may hold values from -4 to 4
- query_feats: bfloat16 [4, 4096, 192], P(('groups', 'design'), ('geom', 'head')), parts along dimension 0, may hold values from -6 to 6
- out_grad: bfloat16 [4, 4096, 192], P(('groups', 'design'), ('geom', 'head')), parts along dimension 0, may hold values from -6 to 6
- norm_gain: float32 [192], replicated, may hold values from 0.5 to 1.5
- w_in: bfloat16 [192, 384], replicated, may hold values from -0.4375 to 0.4375
- w_out: bfloat16 [384, 192], replicated, may hold values from -0.3125 to 0.3125
- w_query: bfloat16 [192, 192], replicated, may hold values from -0.4375 to 0.4375
- w_key: bfloat16 [192, 192], replicated, may hold values from -0.4375 to 0.4375
- w_value: bfloat16 [192, 192], replicated, may hold values from -0.4375 to 0.4375
- w_proj: bfloat16 [192, 192], replicated, may hold values from -0.4375 to 0.4375
Outputs:
- attended: bfloat16 [4, 4096, 192], P(('groups', 'design'), ('geom', 'head')), parts along dimension 0
- point_grad: bfloat16 [4, 12288, 192], P(('groups', 'design'), ('geom', 'head')), parts along dimension 0
- grad_in: float32 [384, 384], P('groups'), parts along dimension 0
- grad_out: float32 [768, 192], P('groups'), parts along dimension 0
- grad_query: float32 [384, 192], P('groups'), parts along dimension 0
- grad_key: float32 [384, 192], P('groups'), parts along dimension 0
- grad_value: float32 [384, 192], P('groups'), parts along dimension 0
- grad_proj: float32 [384, 192], P('groups'), parts along dimension 0
- grad_gain: float32 [384], P('groups'), parts along dimension 0
The draws below stay inside these ranges and needn't reach their ends.
There are 2 independent parts, one for each index of `groups`. The reference program is written for one: setup_inputs(seed, part) draws one part's arguments, and reference() takes and returns one part's arrays. A program takes and returns all parts, laid end to end along the dimension named above; an argument that names none is the same for every part. Nothing has to cross between parts.
Inputs may be any that keep to these rules, and one draw needn't show every extreme that they name: `block_anchor`: block index // 12 is the device that holds the block. Each device assigns at most 2 of its blocks to anchors of any one owner (anchor // 16); in every design one owner gets exactly 2 blocks from every device.
All inputs are finite; a program needn't handle non-finite values.
Results may differ from the reference program's by a relative error of at most 0.03.
Values may be sent and summed in bfloat16 or wider, within the bound.
No kernel may reach another device: no remote copies, remote signals or barrier semaphores. Data moves between devices by JAX's collectives and lax.ppermute only.
A program may use at most 64 MiB of HBM per device.

```python
import jax
import jax.numpy as jnp
from jax import lax

D = 192
HEADS = 3
HID = 384
PB = 128
CAP = 2
BLK_DEV = 12
A_DEV = 16
OWNERS = 8
DESIGNS = 2
BLOCKS = 96
PTS = 12288
ANCH = 128
QRY = 4096


def shuffled(keys_batch, length):

    def one_row(row_key):
        return jax.random.permutation(row_key, length)
    return jax.vmap(one_row)(keys_batch)


def draw_block_anchor(key, part):
    split_keys = jax.random.split(jax.random.fold_in(key, 7), 4)
    hot_owner = jax.random.randint(split_keys[0], (DESIGNS, 1, 1), 0, OWNERS)
    others = shuffled(jax.random.split(split_keys[1], DESIGNS * OWNERS), OWNERS - 1).reshape(DESIGNS, OWNERS, OWNERS - 1)
    block_index = jnp.arange(BLK_DEV)
    pick_index = jnp.broadcast_to(jnp.maximum(block_index - CAP, 0) // CAP, (DESIGNS, OWNERS, BLK_DEV))
    other_owner = (hot_owner + 1 + jnp.take_along_axis(others, pick_index, axis=2)) % OWNERS
    target = jnp.where(block_index < CAP, hot_owner, other_owner)
    shuffle_order = shuffled(jax.random.split(split_keys[2], DESIGNS * OWNERS), BLK_DEV).reshape(DESIGNS, OWNERS, BLK_DEV)
    target = jnp.take_along_axis(target, shuffle_order, axis=2)
    within = jax.random.randint(split_keys[3], (DESIGNS, OWNERS, BLK_DEV), 0, A_DEV)
    return (target * A_DEV + within).reshape(DESIGNS, BLOCKS).astype(jnp.int32)


def block_levels(own_key, extent, cuts, low, largest):
    loudness = 1.0
    for position, blocks in cuts:
        steps = jax.random.uniform(jax.random.fold_in(jax.random.fold_in(own_key, 6), position), (blocks,), jnp.float32, low / len(cuts), largest / len(cuts))
        loudness = loudness * jnp.repeat(jnp.exp(steps), extent[position] // blocks).reshape((-1,) + (1,) * (len(extent) - 1 - position))
    return loudness


def normal_values(stream_key, shape, scale, reach, shards=(), held_as=jnp.bfloat16):
    array = scale * jax.random.normal(stream_key, shape, jnp.float32)
    if shards:
        array = array * block_levels(stream_key, shape, shards, -0.22, 0.18)
    return jnp.clip(array, -reach, reach).astype(held_as)


def setup_inputs(seed: int = 0, part: int = 0) -> dict:
    seeds = jax.random.split(jax.random.key(seed), 13)
    part_keys = jax.random.split(jax.random.fold_in(seeds[12], part), 13)
    point_feats = normal_values(part_keys[0], (DESIGNS, PTS, D), 1.0, 6.0, ((0, 2), (1, 8)))
    block_anchor = draw_block_anchor(jax.random.fold_in(jax.random.fold_in(seeds[12], part), 71), part)
    anchor_feats = normal_values(part_keys[2], (DESIGNS, ANCH, D), 0.3, 4.0, ((0, 2), (1, 8)))
    query_feats = normal_values(part_keys[3], (DESIGNS, QRY, D), 1.0, 6.0, ((0, 2), (1, 8)))
    out_grad = normal_values(part_keys[4], (DESIGNS, QRY, D), 1.0, 6.0, ((0, 2), (1, 8)))
    norm_gain = jnp.clip(1.0 + 0.1 * jax.random.normal(seeds[5], (D,), jnp.float32), 0.5, 1.5)
    w_in = normal_values(seeds[6], (D, HID), D ** -0.5, 0.4375)
    w_out = normal_values(seeds[7], (HID, D), HID ** -0.5, 0.3125)
    w_query = normal_values(seeds[8], (D, D), D ** -0.5, 0.4375)
    w_key = normal_values(seeds[9], (D, D), D ** -0.5, 0.4375)
    w_value = normal_values(seeds[10], (D, D), D ** -0.5, 0.4375)
    w_proj = normal_values(seeds[11], (D, D), D ** -0.5, 0.4375)
    return {"point_feats": point_feats, "block_anchor": block_anchor, "anchor_feats": anchor_feats, "query_feats": query_feats, "out_grad": out_grad, "norm_gain": norm_gain, "w_in": w_in, "w_out": w_out, "w_query": w_query, "w_key": w_key, "w_value": w_value, "w_proj": w_proj}


def gelu_tanh(values):
    return jax.nn.gelu(values, approximate=True)

def contract_rows(first_arg, second_arg, precision=None):
    return lax.dot_general(first_arg.astype(jnp.float32), second_arg.astype(jnp.float32), (((0,), (0,)), ((), ())), precision=precision, preferred_element_type=jnp.float32)

def times_transposed(first_arg, second_arg):
    return lax.dot_general(first_arg.astype(jnp.float32), second_arg.astype(jnp.float32), (((1,), (1,)), ((), ())), preferred_element_type=jnp.float32)

def head_split(matrix):
    return matrix.reshape(matrix.shape[0], HEADS, matrix.shape[1] // HEADS).astype(jnp.float32)

def reference(point_feats, block_anchor, anchor_feats, query_feats, out_grad, norm_gain, w_in, w_out, w_query, w_key, w_value, w_proj):
    exact_mode = lax.Precision.HIGHEST

    def per_design(inputs):
        points, assigned, anchor_rows, query_rows, cotangent = inputs
        feature_width = points.shape[1]
        hidden_width = w_in.shape[1]
        pre_act = jnp.dot(points, w_in, preferred_element_type=jnp.float32)
        hidden = gelu_tanh(pre_act).astype(jnp.bfloat16)
        message = jnp.dot(hidden, w_out, preferred_element_type=jnp.float32)
        block_sums = message.reshape(BLOCKS, PB, feature_width).sum(axis=1)
        member = (jnp.arange(ANCH, dtype=jnp.int32)[:, None] == assigned[None, :]).astype(jnp.float32)
        pooled = jnp.dot(member, block_sums, precision=exact_mode)
        divisor = jnp.maximum(lax.optimization_barrier(jnp.sum(member, axis=1)) * PB, 1.0)
        anchor_sum = anchor_rows.astype(jnp.float32) + pooled / divisor[:, None]
        inv_rms = lax.rsqrt(lax.optimization_barrier(jnp.mean(anchor_sum * anchor_sum, axis=1, keepdims=True)) + 1e-06)
        normed = (anchor_sum * inv_rms * norm_gain).astype(jnp.bfloat16)
        all_keys = jnp.dot(normed, w_key, preferred_element_type=jnp.float32).astype(jnp.bfloat16)
        all_values = jnp.dot(normed, w_value, preferred_element_type=jnp.float32).astype(jnp.bfloat16)
        query_proj = jnp.dot(query_rows, w_query, preferred_element_type=jnp.float32).astype(jnp.bfloat16)
        score_scale = 1.0 / (feature_width // HEADS) ** 0.5
        query_heads = head_split(query_proj)
        key_heads = head_split(all_keys)
        value_heads = head_split(all_values)
        scores = jnp.einsum('qhd,khd->hqk', query_heads, key_heads) * score_scale
        softmax_w = jax.nn.softmax(scores, axis=-1)
        softmax_bf = softmax_w.astype(jnp.bfloat16)
        mixed_heads = jnp.einsum('hqk,khd->qhd', softmax_bf.astype(jnp.float32), value_heads).reshape(-1, feature_width).astype(jnp.bfloat16)
        attended = jnp.dot(mixed_heads, w_proj, preferred_element_type=jnp.float32).astype(jnp.bfloat16)
        grad_proj = contract_rows(mixed_heads, cotangent)
        d_mixed = times_transposed(cotangent, w_proj).astype(jnp.bfloat16)
        dmix_heads = head_split(d_mixed)
        d_probs = jnp.einsum('qhd,khd->hqk', dmix_heads, value_heads)
        d_scores = (softmax_w * (d_probs - lax.optimization_barrier(jnp.sum(softmax_w * d_probs, axis=-1, keepdims=True))) * score_scale).astype(jnp.bfloat16)
        d_query = jnp.einsum('hqk,khd->qhd', d_scores.astype(jnp.float32), key_heads).reshape(-1, feature_width).astype(jnp.bfloat16)
        key_grad = jnp.einsum('hqk,qhd->khd', d_scores.astype(jnp.float32), query_heads).reshape(-1, feature_width).astype(jnp.bfloat16)
        value_grad = jnp.einsum('hqk,qhd->khd', softmax_bf.astype(jnp.float32), dmix_heads).reshape(-1, feature_width).astype(jnp.bfloat16)
        grad_query = contract_rows(query_rows, d_query)
        grad_key = contract_rows(normed, key_grad)
        grad_value = contract_rows(normed, value_grad)
        d_normed = times_transposed(key_grad, w_key) + times_transposed(value_grad, w_value)
        scaled = d_normed * norm_gain
        grad_gain = lax.optimization_barrier(jnp.sum(d_normed * anchor_sum * inv_rms, axis=0))
        d_sum = inv_rms * scaled - anchor_sum * inv_rms ** 3 * lax.optimization_barrier(jnp.mean(scaled * anchor_sum, axis=1, keepdims=True))
        d_pooled = d_sum / divisor[:, None]
        block_grad = contract_rows(member, d_pooled, exact_mode).astype(jnp.bfloat16)
        d_hidden_block = times_transposed(block_grad, w_out)
        d_hidden = jnp.broadcast_to(d_hidden_block[:, None, :], (BLOCKS, PB, hidden_width)).reshape(-1, hidden_width)
        unused_out, gelu_back = jax.vjp(gelu_tanh, pre_act)
        d_pre = gelu_back(d_hidden)[0].astype(jnp.bfloat16)
        hidden_sum = lax.optimization_barrier(jnp.sum(hidden.astype(jnp.float32).reshape(BLOCKS, PB, hidden_width), axis=1))
        grad_out = contract_rows(hidden_sum, block_grad, exact_mode)
        grad_in = contract_rows(points, d_pre)
        point_grad = times_transposed(d_pre, w_in).astype(jnp.bfloat16)
        return (attended, point_grad, (grad_in, grad_out, grad_query, grad_key, grad_value, grad_proj, grad_gain))
    attended, point_grad, stacked = lax.map(per_design, (point_feats, block_anchor, anchor_feats, query_feats, out_grad))
    totals = [lax.optimization_barrier(jnp.sum(member_grad, axis=0)) for member_grad in stacked]
    return (attended, point_grad, totals[0], totals[1], totals[2], totals[3], totals[4], totals[5], totals[6])
```

```python
import functools

import jax
import jax.numpy as jnp
from jax import lax
from jax.experimental import pallas as pl
from jax.experimental.pallas import tpu as pltpu
from jax.sharding import PartitionSpec as P

HEADS = 3
LANES = 128
DIGIT = 128
INTERPRET = False
BF = jnp.bfloat16
F32 = jnp.float32
GELU_C = 0.7978845608028654
GELU_A = 0.044715


def dg(a, b, ca, cb):
    return lax.dot_general(a, b, (((ca,), (cb,)), ((), ())), preferred_element_type=F32)


def split_bf(x):
    high = x.astype(BF)
    return high, (x - high.astype(F32)).astype(BF)


def call(kernel, outs, *args, scratch=(), smem=0):
    specs = [pl.BlockSpec(memory_space=pltpu.SMEM)] * smem
    specs += [pl.BlockSpec(memory_space=pltpu.VMEM)] * (len(args) - smem)
    return pl.pallas_call(
        kernel,
        out_shape=[jax.ShapeDtypeStruct(shape, dtype) for shape, dtype in outs],
        in_specs=specs,
        out_specs=[pl.BlockSpec(memory_space=pltpu.VMEM)] * len(outs),
        scratch_shapes=list(scratch),
        interpret=INTERPRET,
    )(*args)


def round_up(n, k):
    return (n + k - 1) // k * k


def iota(shape, dim):
    return lax.broadcasted_iota(jnp.int32, shape, dim)


def pool_kernel(blocks, x_ref, win_ref, wout_ref, anchor_ref, id_ref, send_ref, slope_ref, hsum_ref):
    width, points = x_ref.shape
    size = points // blocks
    hid = win_ref.shape[1]
    owners, rows, _ = send_ref.shape
    win = win_ref[...]
    step = 2 if blocks % 2 == 0 else 1
    hsum = jnp.zeros((round_up(blocks, 8), hid), F32)
    for first in range(0, blocks, step):
        cols = pl.ds(first * size, step * size)
        pre = dg(win, x_ref[:, cols], 0, 0)
        square = pre * pre
        tanh = jnp.tanh(pre * (GELU_C + (GELU_C * GELU_A) * square))
        half = 0.5 + 0.5 * tanh
        hidden = (pre * half).astype(BF)
        slope = half + pre * ((half * (1.0 - tanh)) * (GELU_C + (3.0 * GELU_C * GELU_A) * square))
        slope_ref[:, cols] = slope.astype(slope_ref.dtype)
        shape = (hsum.shape[0], step * size)
        pick = (iota(shape, 0) == first + iota(shape, 1) // size).astype(F32).astype(BF)
        hsum = hsum + dg(pick, hidden, 1, 1)
    hsum_ref[...] = hsum
    high, low = split_bf(hsum)
    wout = wout_ref[...]
    sums = dg(high, wout, 1, 1) + dg(low, wout, 1, 1)
    ids = id_ref[...]
    digits = jnp.concatenate([ids % DIGIT, ids // DIGIT], axis=0).astype(F32)
    packed = jnp.zeros((rows, 2 * width), F32)
    packed = jnp.concatenate(
        [
            jnp.concatenate(
                [anchor_ref[...].astype(F32)]
                + ([jnp.zeros((rows - anchor_ref.shape[0], width), F32)] if rows > anchor_ref.shape[0] else []),
                axis=0,
            ),
            jnp.concatenate(
                [
                    sums[:blocks],
                    jnp.concatenate([digits, jnp.zeros((2, width - blocks), F32)], axis=1),
                    jnp.zeros((rows - blocks - 2, width), F32),
                ],
                axis=0,
            ),
        ],
        axis=1,
    ).astype(BF)
    for owner in range(owners):
        send_ref[owner] = packed


def query_kernel(x_ref, g_ref, wq_ref, wp_ref, q_ref, dmix_ref):
    q_ref[...] = dg(wq_ref[...], x_ref[...], 0, 0).astype(BF)
    dmix_ref[...] = dg(wp_ref[...], g_ref[...], 1, 0).astype(BF)


def attend_kernel(
    blocks, size, per_owner,
    got_ref, gain_ref, wk_ref, wv_ref, q_ref, dmix_ref,
    rows_ref, normed_ref, k_ref, v_ref, p_ref, ds_ref, kt_ref, vt_ref, gain_out_ref,
):
    owners, rows, both = got_ref.shape
    width = both // 2
    total = owners * rows
    anchors = owners * per_owner
    got = got_ref[...].astype(F32)
    side = got[:, :, width:]
    sums = side.reshape(total, width)
    low = jnp.broadcast_to(side[:, blocks : blocks + 1, :], side.shape).reshape(total, width)
    high = jnp.broadcast_to(side[:, blocks + 1 : blocks + 2, :], side.shape).reshape(total, width)
    lane = iota((total, width), 1)
    place = iota((total, width), 0) % rows
    ids = jnp.sum(jnp.where(lane == place, low + high * DIGIT, 0.0), axis=1, keepdims=True)
    valid = (iota((total, 1), 0) % rows) < blocks
    ids = jnp.where(valid, ids, -1.0).astype(jnp.int32)
    member = (ids == iota((total, anchors), 1)).astype(F32).astype(BF)
    sums_bf = sums.astype(BF)
    pooled = dg(member, sums_bf, 0, 0)
    count = dg(member, jnp.ones((total, LANES), BF), 0, 0)[:, :1]
    inv_div = 1.0 / jnp.maximum(count * size, 1.0)
    anchor_rows = got[:, :per_owner, :width].reshape(anchors, width)
    asum = anchor_rows + pooled * inv_div
    inv = lax.rsqrt(jnp.mean(asum * asum, axis=1, keepdims=True) + 1e-6)
    gain = gain_ref[...]
    unit = asum * inv
    normed = (unit * gain).astype(BF)
    normed_ref[...] = normed
    keys = dg(wk_ref[...], normed, 0, 1).astype(BF)
    values = dg(wv_ref[...], normed, 0, 1).astype(BF)
    k_ref[...] = keys
    v_ref[...] = values
    depth = width // HEADS
    scale = 1.0 / depth**0.5
    for head in range(HEADS):
        part = slice(head * depth, (head + 1) * depth)
        q = q_ref[part, :]
        dmix = dmix_ref[part, :]
        scores = dg(keys[part], q, 0, 0) * scale
        top = jnp.max(scores, axis=0, keepdims=True)
        weight = jnp.exp(scores - top)
        probs = weight * (1.0 / jnp.sum(weight, axis=0, keepdims=True))
        probs_bf = probs.astype(BF)
        p_ref[head] = probs_bf
        dprobs = dg(values[part], dmix, 0, 0)
        inner = jnp.sum(probs * dprobs, axis=0, keepdims=True)
        dscore = (probs * (dprobs - inner) * scale).astype(BF)
        ds_ref[head] = dscore
        kt_ref[part, :] = dg(q, dscore, 1, 1).astype(BF)
        vt_ref[part, :] = dg(dmix, probs_bf, 1, 1).astype(BF)
    dnorm = dg(kt_ref[...], wk_ref[...], 0, 1) + dg(vt_ref[...], wv_ref[...], 0, 1)
    gain_out_ref[...] = jnp.sum(dnorm * unit, axis=0, keepdims=True)
    scaled = dnorm * gain
    dsum = inv * scaled - asum * (inv * inv * inv) * jnp.mean(scaled * asum, axis=1, keepdims=True)
    dpool = (dsum * inv_div).astype(BF)
    rows_ref[...] = dg(member, dpool, 1, 0).astype(BF).reshape(owners, rows, width)


def put_rows(ref, chunk, start, value):
    done = 0
    while done < value.shape[0]:
        index, offset = divmod(start + done, chunk)
        take = min(chunk - offset, value.shape[0] - done)
        ref[index, offset : offset + take, :] = value[done : done + take]
        done += take


def get_rows(read, chunk, start, count):
    pieces = []
    done = 0
    while done < count:
        index, offset = divmod(start + done, chunk)
        take = min(chunk - offset, count - done)
        pieces.append(read(index, offset, take))
        done += take
    return pieces[0] if len(pieces) == 1 else jnp.concatenate(pieces, axis=0)


def pack_square(ref, chunk, mats, start):
    width = mats[0].shape[0]
    for mat in mats:
        put_rows(ref, chunk, start, mat[:, :LANES])
        start += width
    for first in range(0, len(mats), 2):
        pair = jnp.concatenate([mats[first][:, LANES:], mats[first + 1][:, LANES:]], axis=1)
        put_rows(ref, chunk, start, pair)
        start += width
    return start


def swap_halves(head_ref, scratch, keep_ref, send_ref):
    half = keep_ref.shape[0]
    head = head_ref[0]
    keep_ref[...] = scratch[pl.ds(head * half, half)].astype(keep_ref.dtype)
    send_ref[...] = scratch[pl.ds((1 - head) * half, half)].astype(send_ref.dtype)


def finish_kernel(
    chunk, head_ref, p_ref, ds_ref, k_ref, v_ref, kt_ref, vt_ref, normed_ref, gain_ref, x_ref, g_ref,
    wp_ref, out_ref, keep_ref, send_ref, mixed_ref, dq_ref, pack_ref,
):
    width = k_ref.shape[0]
    depth = width // HEADS
    for head in range(HEADS):
        part = slice(head * depth, (head + 1) * depth)
        mixed_ref[part, :] = dg(v_ref[part, :], p_ref[head], 1, 0).astype(BF)
        dq_ref[part, :] = dg(k_ref[part, :], ds_ref[head], 1, 0).astype(BF)
    mixed = mixed_ref[...]
    out_ref[...] = dg(wp_ref[...], mixed, 0, 0).astype(BF)
    mats = [
        dg(x_ref[...], dq_ref[...], 1, 1),
        dg(normed_ref[...], kt_ref[...], 0, 1),
        dg(normed_ref[...], vt_ref[...], 0, 1),
        dg(mixed, g_ref[...], 1, 1),
    ]
    pieces, rows, _ = pack_ref.shape
    pack_square(pack_ref, chunk, mats, 0)
    gain = gain_ref[...]
    pack_ref[:, chunk:, :] = jnp.zeros((pieces, rows - chunk, LANES), F32)
    pack_ref[0, chunk : chunk + 1, :] = gain[:, :LANES]
    rest = width - LANES
    pack_ref[0, chunk + 1 : chunk + 2, :] = jnp.concatenate(
        [gain[:, LANES:], jnp.zeros((1, LANES - rest), F32)], axis=1
    )
    swap_halves(head_ref, pack_ref, keep_ref, send_ref)


def back_kernel(
    blocks, chunk, head_ref, got_ref, wout_ref, slope_ref, x_ref, hsum_ref,
    dpre_ref, keep_ref, send_ref, pack_ref,
):
    width, points = x_ref.shape
    size = points // blocks
    grad = jnp.sum(got_ref[...].astype(F32), axis=0)[: hsum_ref.shape[0]].astype(BF)
    dhid = dg(wout_ref[...], grad, 0, 1)
    for block in range(blocks):
        cols = pl.ds(block * size, size)
        dpre_ref[:, cols] = (slope_ref[:, cols].astype(F32) * dhid[:, block : block + 1]).astype(BF)
    gin = dg(x_ref[...], dpre_ref[...], 1, 1)
    high, low = split_bf(hsum_ref[...])
    gout = dg(grad, high, 0, 0) + dg(grad, low, 0, 0)
    start = 0
    for mat in (gin, gout):
        for lane in range(0, mat.shape[1], LANES):
            put_rows(pack_ref, chunk, start, mat[:, lane : lane + LANES])
            start += width
    swap_halves(head_ref, pack_ref, keep_ref, send_ref)


def point_grad_kernel(win_ref, dpre_ref, out_ref):
    out_ref[...] = dg(win_ref[...], dpre_ref[...], 1, 0).astype(BF)


def join_kernel(ka_ref, ra_ref, kp_ref, rp_ref, out_ref):
    rows = ka_ref.shape[1]
    out_ref[:, :rows, :] = (ka_ref[...] + ra_ref[...].astype(F32)).astype(BF)
    out_ref[:, rows:, :] = (kp_ref[...] + rp_ref[...].astype(F32)).astype(BF)


def sum_kernel(got_ref, out_ref):
    total = jnp.sum(got_ref[...].astype(F32), axis=0).astype(BF)
    for peer in range(out_ref.shape[0]):
        out_ref[peer] = total


def unpack_kernel(
    chunk_a, rows_a, chunk_p, head_ref, mine_ref, other_ref,
    gin_ref, gout_ref, gq_ref, gk_ref, gv_ref, gp_ref, gain_ref, all_ref,
):
    peers = mine_ref.shape[0]
    head = head_ref[0]
    all_ref[pl.ds(head * peers, peers)] = mine_ref[...]
    all_ref[pl.ds((1 - head) * peers, peers)] = other_ref[...]

    def read_a(index, offset, take):
        return all_ref[index, offset : offset + take, :].astype(F32)

    def read_p(index, offset, take):
        return all_ref[index, rows_a + offset : rows_a + offset + take, :].astype(F32)

    width = gq_ref.shape[0]
    squares = (gq_ref, gk_ref, gv_ref, gp_ref)
    start = 0
    for ref in squares:
        ref[:, :LANES] = get_rows(read_a, chunk_a, start, width)
        start += width
    rest = width - LANES
    for first in range(0, len(squares), 2):
        pair = get_rows(read_a, chunk_a, start, width)
        squares[first][:, LANES:] = pair[:, :rest]
        squares[first + 1][:, LANES:] = pair[:, rest:]
        start += width
    tail = all_ref[0, chunk_a:rows_a, :].astype(F32)
    gain_ref[...] = jnp.concatenate([tail[:1], tail[1:2, :rest]], axis=1)
    start = 0
    for ref in (gin_ref, gout_ref):
        for lane in range(0, ref.shape[1], LANES):
            ref[:, lane : lane + LANES] = get_rows(read_p, chunk_p, start, width)
            start += width


def on_device(
    point_feats, block_anchor, anchor_feats, query_feats, out_grad, norm_gain,
    w_in, w_out, w_query, w_key, w_value, w_proj,
):
    team = ("geom", "head")
    crowd = ("geom", "design")
    owners = lax.axis_size(team)
    peers = lax.axis_size(crowd)
    xt = point_feats[0].T
    qt = query_feats[0].T
    gt = out_grad[0].T
    wot = w_out.T
    blocks = block_anchor.shape[1]
    per_owner, width = anchor_feats.shape[1:]
    points = xt.shape[1]
    queries = qt.shape[1]
    hid = w_in.shape[1]
    size = points // blocks
    anchors = owners * per_owner
    rows = round_up(max(per_owner, blocks + 2), 16)
    head = lax.axis_index("head").astype(jnp.int32).reshape(1)
    pieces = 2 * peers
    chunk_a = 6 * width // pieces
    rows_a = chunk_a + 8
    chunk_p = 2 * width * hid // LANES // pieces

    send, slope, hsum = call(
        functools.partial(pool_kernel, blocks),
        [((owners, rows, 2 * width), BF), ((hid, points), BF), ((round_up(blocks, 8), hid), F32)],
        xt, w_in, wot, anchor_feats[0], block_anchor,
    )
    got = lax.all_to_all(send, team, 0, 0, tiled=True)
    qp, dmix = call(
        query_kernel, [((width, queries), BF), ((width, queries), BF)], qt, gt, w_query, w_proj
    )
    pair_shape = (HEADS, anchors, queries)
    rows_out, normed, keys, values, probs, dscore, kt, vt, gain_part = call(
        functools.partial(attend_kernel, blocks, size, per_owner),
        [
            ((owners, rows, width), BF),
            ((anchors, width), BF),
            ((width, anchors), BF),
            ((width, anchors), BF),
            (pair_shape, BF),
            (pair_shape, BF),
            ((width, anchors), BF),
            ((width, anchors), BF),
            ((1, width), F32),
        ],
        got, norm_gain.reshape(1, width), w_key, w_value, qp, dmix,
    )
    back = lax.all_to_all(rows_out, team, 0, 0, tiled=True)
    attended, keep_a, send_a = call(
        functools.partial(finish_kernel, chunk_a),
        [((width, queries), BF), ((peers, rows_a, LANES), F32), ((peers, rows_a, LANES), BF)],
        head, probs, dscore, keys, values, kt, vt, normed, gain_part, qt, gt, w_proj,
        scratch=[
            pltpu.VMEM((width, queries), BF),
            pltpu.VMEM((width, queries), BF),
            pltpu.VMEM((pieces, rows_a, LANES), F32),
        ],
        smem=1,
    )
    swap = [(0, 1), (1, 0)]
    recv_a = lax.ppermute(send_a, "head", swap)
    dpre, keep_p, send_p = call(
        functools.partial(back_kernel, blocks, chunk_p),
        [((hid, points), BF), ((peers, chunk_p, LANES), F32), ((peers, chunk_p, LANES), BF)],
        head, back, wot, slope, xt, hsum,
        scratch=[pltpu.VMEM((pieces, chunk_p, LANES), F32)],
        smem=1,
    )
    recv_p = lax.ppermute(send_p, "head", swap)
    (joined,) = call(join_kernel, [((peers, rows_a + chunk_p, LANES), BF)], keep_a, recv_a, keep_p, recv_p)
    scattered = lax.all_to_all(joined, crowd, 0, 0, tiled=True)
    (point_grad,) = call(point_grad_kernel, [((width, points), BF)], w_in, dpre)
    (summed,) = call(sum_kernel, [((peers, rows_a + chunk_p, LANES), BF)], scattered)
    mine = lax.all_to_all(summed, crowd, 0, 0, tiled=True)
    other = lax.ppermute(mine, "head", swap)
    square = ((width, width), F32)
    gin, gout, gq, gk, gv, gp, gain = call(
        functools.partial(unpack_kernel, chunk_a, rows_a, chunk_p),
        [((width, hid), F32), ((width, hid), F32), square, square, square, square, ((1, width), F32)],
        head, mine, other,
        scratch=[pltpu.VMEM((pieces, rows_a + chunk_p, LANES), BF)],
        smem=1,
    )
    return (
        attended.T[None], point_grad.T[None], gin, gout.T, gq, gk, gv, gp, gain.reshape(width),
    )


def solution(mesh):
    split = P(("groups", "design"), ("geom", "head"), None)
    placed = (split, P(("groups", "design"), ("geom", "head")), split, split, split) + (P(),) * 7
    grads = (P("groups", None),) * 6 + (P("groups"),)
    return jax.shard_map(
        on_device, mesh=mesh, in_specs=placed, out_specs=(split, split) + grads, check_vma=False
    )
```

```python
import functools

import jax
import jax.numpy as jnp
from jax import lax
from jax.experimental import pallas as pl
from jax.experimental.pallas import tpu as pltpu
from jax.sharding import PartitionSpec as P

HEADS = 3
LANES = 128
DIGIT = 128
INTERPRET = False
VMEM_LIMIT = 24 << 20
BF = jnp.bfloat16
F32 = jnp.float32
GELU_C = 0.7978845608028654
GELU_A = 0.044715


def dg(a, b, ca, cb):
    return lax.dot_general(a, b, (((ca,), (cb,)), ((), ())), preferred_element_type=F32)


def split_bf(x):
    high = x.astype(BF)
    return high, (x - high.astype(F32)).astype(BF)


class Held:
    def __init__(self, value, space):
        self.value, self.space = value, space


def near(*values):
    return tuple(Held(value, pltpu.VMEM) for value in values)


def call(kernel, outs, *args, scratch=(), smem=0, final=(), raw=()):
    held = [Held(arg, None) for arg in args[:smem]]
    held += [arg if isinstance(arg, Held) else Held(arg, pltpu.HBM) for arg in args[smem:]]
    specs = [pl.BlockSpec(memory_space=pltpu.SMEM)] * smem
    for arg in held[smem:]:
        near_spec = pl.BlockSpec(memory_space=pltpu.VMEM)
        specs.append(near_spec if arg.space is pltpu.VMEM else pl.BlockSpec())
    held += [arg if isinstance(arg, Held) else Held(arg, pltpu.HBM) for arg in raw]
    specs += [pl.BlockSpec(memory_space=pl.ANY)] * len(raw)
    operands = [
        arg.value
        if INTERPRET or arg.space is None
        else pltpu.with_memory_space_constraint(arg.value, arg.space)
        for arg in held
    ]
    return pl.pallas_call(
        kernel,
        out_shape=[
            jax.ShapeDtypeStruct(shape, dtype)
            if INTERPRET
            else (pltpu.HBM if place in final else pltpu.VMEM)(shape, dtype)
            for place, (shape, dtype) in enumerate(outs)
        ],
        in_specs=specs,
        out_specs=[
            pl.BlockSpec() if place in final else pl.BlockSpec(memory_space=pltpu.VMEM)
            for place in range(len(outs))
        ],
        scratch_shapes=list(scratch),
        compiler_params=pltpu.CompilerParams(vmem_limit_bytes=VMEM_LIMIT),
        interpret=INTERPRET,
    )(*operands)


def round_up(n, k):
    return (n + k - 1) // k * k


def iota(shape, dim):
    return lax.broadcasted_iota(jnp.int32, shape, dim)


def gelu_terms(win, x):
    pre = dg(win, x, 0, 0)
    square = pre * pre
    tanh = jnp.tanh(pre * (GELU_C + (GELU_C * GELU_A) * square))
    return pre, square, tanh


def pool_kernel(blocks, x_ref, win_ref, wout_ref, anchor_ref, id_ref, send_ref, hsum_ref):
    width, points = x_ref.shape
    size = points // blocks
    hid = win_ref.shape[1]
    owners, rows, _ = send_ref.shape
    win = win_ref[...]
    step = 2 if blocks % 2 == 0 else 1
    hsum = jnp.zeros((round_up(blocks, 8), hid), F32)
    for first in range(0, blocks, step):
        pre, _, tanh = gelu_terms(win, x_ref[:, pl.ds(first * size, step * size)])
        half = 0.5 * pre
        hidden = (half + half * tanh).astype(BF)
        shape = (hsum.shape[0], step * size)
        pick = (iota(shape, 0) == first + iota(shape, 1) // size).astype(F32).astype(BF)
        hsum = hsum + dg(pick, hidden, 1, 1)
    hsum_ref[...] = hsum
    high, low = split_bf(hsum)
    wout = wout_ref[...]
    sums = dg(high, wout, 1, 1) + dg(low, wout, 1, 1)
    ids = id_ref[...]
    digits = jnp.concatenate([ids % DIGIT, ids // DIGIT], axis=0).astype(F32)
    packed = jnp.zeros((rows, 2 * width), F32)
    packed = jnp.concatenate(
        [
            jnp.concatenate(
                [anchor_ref[...].astype(F32)]
                + ([jnp.zeros((rows - anchor_ref.shape[0], width), F32)] if rows > anchor_ref.shape[0] else []),
                axis=0,
            ),
            jnp.concatenate(
                [
                    sums[:blocks],
                    jnp.concatenate([digits, jnp.zeros((2, width - blocks), F32)], axis=1),
                    jnp.zeros((rows - blocks - 2, width), F32),
                ],
                axis=0,
            ),
        ],
        axis=1,
    ).astype(BF)
    for owner in range(owners):
        send_ref[owner] = packed


def query_kernel(
    blocks, x_ref, g_ref, wq_ref, wp_ref, wk_ref, wv_ref, gain_ref, xp_ref, win_ref,
    q_ref, dmix_ref, wk_out, wv_out, gain_out, slope_ref,
):
    wk_out[...] = wk_ref[...]
    wv_out[...] = wv_ref[...]
    gain_out[...] = gain_ref[...]
    q_ref[...] = dg(wq_ref[...], x_ref[...], 0, 0).astype(BF)
    dmix_ref[...] = dg(wp_ref[...], g_ref[...], 1, 0).astype(BF)
    win = win_ref[...]
    points = xp_ref.shape[1]
    step = points // blocks * (2 if blocks % 2 == 0 else 1)
    for first in range(0, points, step):
        pre, square, tanh = gelu_terms(win, xp_ref[:, pl.ds(first, step)])
        half = 0.5 + 0.5 * tanh
        slope = half + pre * ((half * (1.0 - tanh)) * (GELU_C + (3.0 * GELU_C * GELU_A) * square))
        slope_ref[:, pl.ds(first, step)] = slope.astype(BF)


def attend_kernel(
    blocks, size, per_owner,
    got_ref, gain_ref, wk_ref, wv_ref, q_ref, dmix_ref,
    rows_ref, normed_ref, k_ref, v_ref, p_ref, ds_ref, kt_ref, vt_ref, gain_out_ref,
):
    owners, rows, both = got_ref.shape
    width = both // 2
    total = owners * rows
    anchors = owners * per_owner
    got = got_ref[...].astype(F32)
    side = got[:, :, width:]
    sums = side.reshape(total, width)
    low = jnp.broadcast_to(side[:, blocks : blocks + 1, :], side.shape).reshape(total, width)
    high = jnp.broadcast_to(side[:, blocks + 1 : blocks + 2, :], side.shape).reshape(total, width)
    lane = iota((total, width), 1)
    place = iota((total, width), 0) % rows
    ids = jnp.sum(jnp.where(lane == place, low + high * DIGIT, 0.0), axis=1, keepdims=True)
    valid = (iota((total, 1), 0) % rows) < blocks
    ids = jnp.where(valid, ids, -1.0).astype(jnp.int32)
    member = (ids == iota((total, anchors), 1)).astype(F32).astype(BF)
    sums_bf = sums.astype(BF)
    pooled = dg(member, sums_bf, 0, 0)
    count = dg(member, jnp.ones((total, LANES), BF), 0, 0)[:, :1]
    inv_div = 1.0 / jnp.maximum(count * size, 1.0)
    anchor_rows = got[:, :per_owner, :width].reshape(anchors, width)
    asum = anchor_rows + pooled * inv_div
    inv = lax.rsqrt(jnp.mean(asum * asum, axis=1, keepdims=True) + 1e-6)
    gain = gain_ref[...]
    unit = asum * inv
    normed = (unit * gain).astype(BF)
    normed_ref[...] = normed
    keys = dg(wk_ref[...], normed, 0, 1).astype(BF)
    values = dg(wv_ref[...], normed, 0, 1).astype(BF)
    k_ref[...] = keys
    v_ref[...] = values
    depth = width // HEADS
    scale = 1.0 / depth**0.5
    for head in range(HEADS):
        part = slice(head * depth, (head + 1) * depth)
        q = q_ref[part, :]
        dmix = dmix_ref[part, :]
        scores = dg(keys[part], q, 0, 0) * scale
        top = jnp.max(scores, axis=0, keepdims=True)
        weight = jnp.exp(scores - top)
        probs = weight * (1.0 / jnp.sum(weight, axis=0, keepdims=True))
        probs_bf = probs.astype(BF)
        p_ref[head] = probs_bf
        dprobs = dg(values[part], dmix, 0, 0)
        inner = jnp.sum(probs * dprobs, axis=0, keepdims=True)
        dscore = (probs * (dprobs - inner) * scale).astype(BF)
        ds_ref[head] = dscore
        kt_ref[part, :] = dg(q, dscore, 1, 1).astype(BF)
        vt_ref[part, :] = dg(dmix, probs_bf, 1, 1).astype(BF)
    dnorm = dg(kt_ref[...], wk_ref[...], 0, 1) + dg(vt_ref[...], wv_ref[...], 0, 1)
    gain_out_ref[...] = jnp.sum(dnorm * unit, axis=0, keepdims=True)
    scaled = dnorm * gain
    dsum = inv * scaled - asum * (inv * inv * inv) * jnp.mean(scaled * asum, axis=1, keepdims=True)
    dpool = (dsum * inv_div).astype(BF)
    rows_ref[...] = dg(member, dpool, 1, 0).astype(BF).reshape(owners, rows, width)


def put_rows(ref, chunk, start, value):
    done = 0
    while done < value.shape[0]:
        index, offset = divmod(start + done, chunk)
        take = min(chunk - offset, value.shape[0] - done)
        ref[index, offset : offset + take, :] = value[done : done + take]
        done += take


def get_rows(read, chunk, start, count):
    pieces = []
    done = 0
    while done < count:
        index, offset = divmod(start + done, chunk)
        take = min(chunk - offset, count - done)
        pieces.append(read(index, offset, take))
        done += take
    return pieces[0] if len(pieces) == 1 else jnp.concatenate(pieces, axis=0)


def pack_square(ref, chunk, mats, start):
    width = mats[0].shape[0]
    for mat in mats:
        put_rows(ref, chunk, start, mat[:, :LANES])
        start += width
    for first in range(0, len(mats), 2):
        pair = jnp.concatenate([mats[first][:, LANES:], mats[first + 1][:, LANES:]], axis=1)
        put_rows(ref, chunk, start, pair)
        start += width
    return start


def swap_halves(head_ref, scratch, keep_ref, send_ref):
    half = keep_ref.shape[0]
    head = head_ref[0]
    keep_ref[...] = scratch[pl.ds(head * half, half)].astype(keep_ref.dtype)
    send_ref[...] = scratch[pl.ds((1 - head) * half, half)].astype(send_ref.dtype)


def finish_kernel(
    chunk, head_ref, p_ref, ds_ref, k_ref, v_ref, kt_ref, vt_ref, normed_ref, gain_ref, x_ref, g_ref,
    wp_ref, *refs,
):
    count = (len(refs) - 6) // 2
    out_ref, keep_ref, send_ref = refs[count : count + 3]
    mixed_ref, dq_ref, pack_ref, sems = refs[-4:]
    points = refs[0].shape[1]
    both = refs[count + 3]
    targets = [both.at[:, :points], both.at[:, points:]] + list(refs[count + 4 : -4])
    copies = [
        pltpu.make_async_copy(source, target, sems.at[place])
        for place, (source, target) in enumerate(zip(refs[:count], targets))
    ]
    for copy in copies:
        copy.start()
    width = k_ref.shape[0]
    depth = width // HEADS
    for head in range(HEADS):
        part = slice(head * depth, (head + 1) * depth)
        mixed_ref[part, :] = dg(v_ref[part, :], p_ref[head], 1, 0).astype(BF)
        dq_ref[part, :] = dg(k_ref[part, :], ds_ref[head], 1, 0).astype(BF)
    mixed = mixed_ref[...]
    out_ref[...] = dg(wp_ref[...], mixed, 0, 0).astype(BF)
    mats = [
        dg(x_ref[...], dq_ref[...], 1, 1),
        dg(normed_ref[...], kt_ref[...], 0, 1),
        dg(normed_ref[...], vt_ref[...], 0, 1),
        dg(mixed, g_ref[...], 1, 1),
    ]
    pieces, rows, _ = pack_ref.shape
    pack_square(pack_ref, chunk, mats, 0)
    gain = gain_ref[...]
    pack_ref[:, chunk:, :] = jnp.zeros((pieces, rows - chunk, LANES), F32)
    pack_ref[0, chunk : chunk + 1, :] = gain[:, :LANES]
    rest = width - LANES
    pack_ref[0, chunk + 1 : chunk + 2, :] = jnp.concatenate(
        [gain[:, LANES:], jnp.zeros((1, LANES - rest), F32)], axis=1
    )
    swap_halves(head_ref, pack_ref, keep_ref, send_ref)
    for copy in copies:
        copy.wait()


def back_kernel(
    blocks, chunk, head_ref, got_ref, both_ref, slope_ref, hsum_ref, *refs,
):
    dpre_ref, keep_ref, send_ref, pack_ref = refs[-4:]
    width = both_ref.shape[0]
    points = slope_ref.shape[1]
    size = points // blocks
    x_ref = both_ref.at[:, :points]
    wout_ref = both_ref.at[:, points:]
    grad = jnp.sum(got_ref[...].astype(F32), axis=0)[: hsum_ref.shape[0]].astype(BF)
    dhid = dg(wout_ref[...], grad, 0, 1)
    for block in range(blocks):
        cols = pl.ds(block * size, size)
        dpre_ref[:, cols] = (slope_ref[:, cols].astype(F32) * dhid[:, block : block + 1]).astype(BF)
    gin = dg(x_ref[...], dpre_ref[...], 1, 1)
    high, low = split_bf(hsum_ref[...])
    gout = dg(grad, high, 0, 0) + dg(grad, low, 0, 0)
    start = 0
    for mat in (gin, gout):
        for lane in range(0, mat.shape[1], LANES):
            put_rows(pack_ref, chunk, start, mat[:, lane : lane + LANES])
            start += width
    swap_halves(head_ref, pack_ref, keep_ref, send_ref)


def point_grad_kernel(win_ref, dpre_ref, after_ref, out_ref):
    out_ref[...] = dg(win_ref[...], dpre_ref[...], 1, 0).astype(BF)


def join_kernel(ka_ref, ra_ref, kp_ref, rp_ref, after_ref, out_ref):
    rows = ka_ref.shape[1]
    out_ref[:, :rows, :] = (ka_ref[...].astype(F32) + ra_ref[...].astype(F32)).astype(BF)
    out_ref[:, rows:, :] = (kp_ref[...].astype(F32) + rp_ref[...].astype(F32)).astype(BF)


def sum_kernel(got_ref, *refs):
    out_ref = refs[-1]
    total = jnp.sum(got_ref[...].astype(F32), axis=0).astype(BF)
    for peer in range(out_ref.shape[0]):
        out_ref[peer] = total


def unpack_kernel(
    chunk_a, rows_a, chunk_p, head_ref, mine_ref, other_ref,
    gin_ref, gout_ref, gq_ref, gk_ref, gv_ref, gp_ref, gain_ref, all_ref,
):
    peers = mine_ref.shape[0]
    head = head_ref[0]
    all_ref[pl.ds(head * peers, peers)] = mine_ref[...]
    all_ref[pl.ds((1 - head) * peers, peers)] = other_ref[...]

    def read_a(index, offset, take):
        return all_ref[index, offset : offset + take, :].astype(F32)

    def read_p(index, offset, take):
        return all_ref[index, rows_a + offset : rows_a + offset + take, :].astype(F32)

    width = gq_ref.shape[0]
    squares = (gq_ref, gk_ref, gv_ref, gp_ref)
    start = 0
    for ref in squares:
        ref[:, :LANES] = get_rows(read_a, chunk_a, start, width)
        start += width
    rest = width - LANES
    for first in range(0, len(squares), 2):
        pair = get_rows(read_a, chunk_a, start, width)
        squares[first][:, LANES:] = pair[:, :rest]
        squares[first + 1][:, LANES:] = pair[:, rest:]
        start += width
    tail = all_ref[0, chunk_a:rows_a, :].astype(F32)
    gain_ref[...] = jnp.concatenate([tail[:1], tail[1:2, :rest]], axis=1)
    start = 0
    for ref in (gin_ref, gout_ref):
        for lane in range(0, ref.shape[1], LANES):
            ref[:, lane : lane + LANES] = get_rows(read_p, chunk_p, start, width)
            start += width


def on_device(
    point_feats, block_anchor, anchor_feats, query_feats, out_grad, norm_gain,
    w_in, w_out, w_query, w_key, w_value, w_proj,
):
    team = ("geom", "head")
    crowd = ("geom", "design")
    owners = lax.axis_size(team)
    peers = lax.axis_size(crowd)
    xt = point_feats[0].T
    qt = query_feats[0].T
    gt = out_grad[0].T
    wot = w_out.T
    blocks = block_anchor.shape[1]
    per_owner, width = anchor_feats.shape[1:]
    points = xt.shape[1]
    queries = qt.shape[1]
    hid = w_in.shape[1]
    size = points // blocks
    anchors = owners * per_owner
    rows = round_up(max(per_owner, blocks + 2), 16)
    head = lax.axis_index("head").astype(jnp.int32).reshape(1)
    pieces = 2 * peers
    chunk_a = 6 * width // pieces
    rows_a = chunk_a + 8
    chunk_p = 2 * width * hid // LANES // pieces

    send, hsum = call(
        functools.partial(pool_kernel, blocks),
        [((owners, rows, 2 * width), BF), ((round_up(blocks, 8), hid), F32)],
        xt, w_in, wot, anchor_feats[0], block_anchor,
        final=(1,),
    )
    got = lax.all_to_all(send, team, 0, 0, tiled=True)
    qp, dmix, wk, wv, gain_row, slope = call(
        functools.partial(query_kernel, blocks),
        [
            ((width, queries), BF),
            ((width, queries), BF),
            ((width, width), BF),
            ((width, width), BF),
            ((1, width), F32),
            ((hid, points), BF),
        ],
        qt, gt, w_query, w_proj, w_key, w_value, norm_gain.reshape(1, width), xt, w_in,
        final=(5,),
    )
    pair_shape = (HEADS, anchors, queries)
    rows_out, normed, keys, values, probs, dscore, kt, vt, gain_part = call(
        functools.partial(attend_kernel, blocks, size, per_owner),
        [
            ((owners, rows, width), BF),
            ((anchors, width), BF),
            ((width, anchors), BF),
            ((width, anchors), BF),
            (pair_shape, BF),
            (pair_shape, BF),
            ((width, anchors), BF),
            ((width, anchors), BF),
            ((1, width), F32),
        ],
        *near(got, gain_row, wk, wv, qp, dmix),
    )
    back = lax.all_to_all(rows_out, team, 0, 0, tiled=True)
    attended, keep_a, send_a, both, slope, hsum, win = call(
        functools.partial(finish_kernel, chunk_a),
        [
            ((width, queries), BF),
            ((peers, rows_a, LANES), BF),
            ((peers, rows_a, LANES), BF),
            ((width, points + hid), BF),
            ((hid, points), BF),
            (hsum.shape, F32),
            ((width, hid), BF),
        ],
        head, *near(probs, dscore, keys, values, kt, vt, normed, gain_part), qt, gt, w_proj,
        raw=(xt, wot, slope, hsum, w_in),
        scratch=[
            pltpu.VMEM((width, queries), BF),
            pltpu.VMEM((width, queries), BF),
            pltpu.VMEM((pieces, rows_a, LANES), F32),
            pltpu.SemaphoreType.DMA((5,)),
        ],
        smem=1,
        final=(0,),
    )
    swap = [(0, 1), (1, 0)]
    shape_p = ((peers, chunk_p, LANES), BF)
    shape_all = ((peers, rows_a + chunk_p, LANES), BF)
    recv_a = lax.ppermute(send_a, "head", swap)
    dpre, keep_p, send_p = call(
        functools.partial(back_kernel, blocks, chunk_p),
        [((hid, points), BF), shape_p, shape_p],
        head, *near(back, both, slope, hsum),
        scratch=[pltpu.VMEM((pieces, chunk_p, LANES), F32)],
        smem=1,
    )
    recv_p = lax.ppermute(send_p, "head", swap)
    (point_grad,) = call(
        point_grad_kernel, [((width, points), BF)], *near(win, dpre), final=(0,), raw=near(send_p)
    )
    (joined,) = call(
        join_kernel, [shape_all], *near(keep_a, recv_a, keep_p, recv_p), raw=(point_grad,)
    )
    scattered = lax.all_to_all(joined, crowd, 0, 0, tiled=True)
    (summed,) = call(sum_kernel, [shape_all], *near(scattered))
    mine = lax.all_to_all(summed, crowd, 0, 0, tiled=True)
    other = lax.ppermute(mine, "head", swap)
    square = ((width, width), F32)
    gin, gout, gq, gk, gv, gp, gain = call(
        functools.partial(unpack_kernel, chunk_a, rows_a, chunk_p),
        [((width, hid), F32), ((width, hid), F32), square, square, square, square, ((1, width), F32)],
        head, *near(mine, other),
        scratch=[pltpu.VMEM((pieces, rows_a + chunk_p, LANES), BF)],
        smem=1,
        final=range(7),
    )
    return (
        attended.T[None], point_grad.T[None], gin, gout.T, gq, gk, gv, gp, gain.reshape(width),
    )


def solution(mesh):
    split = P(("groups", "design"), ("geom", "head"), None)
    placed = (split, P(("groups", "design"), ("geom", "head")), split, split, split) + (P(),) * 7
    grads = (P("groups", None),) * 6 + (P("groups"),)
    return jax.shard_map(
        on_device, mesh=mesh, in_specs=placed, out_specs=(split, split) + grads, check_vma=False
    )
```

```python
import functools

import jax
import jax.numpy as jnp
from jax import lax
from jax.experimental import pallas as pl
from jax.experimental.pallas import tpu as pltpu
from jax.sharding import PartitionSpec as P


HEADS = 3
LANES = 128
DIGIT = 128
INTERPRET = False
VMEM_LIMIT = 24 << 20
BF = jnp.bfloat16
F32 = jnp.float32
GELU_C = 0.7978845608028654
GELU_A = 0.044715


def dg(a, b, ca, cb):
    return lax.dot_general(a, b, (((ca,), (cb,)), ((), ())), preferred_element_type=F32)


def split_bf(x):
    high = x.astype(BF)
    return high, (x - high.astype(F32)).astype(BF)


class Held:
    def __init__(self, value, space):
        self.value, self.space = value, space


def near(*values):
    return tuple(Held(value, pltpu.VMEM) for value in values)


def call(kernel, outs, *args, scratch=(), smem=0, final=(), raw=()):
    held = [Held(arg, None) for arg in args[:smem]]
    held += [arg if isinstance(arg, Held) else Held(arg, pltpu.HBM) for arg in args[smem:]]
    specs = [pl.BlockSpec(memory_space=pltpu.SMEM)] * smem
    for arg in held[smem:]:
        near_spec = pl.BlockSpec(memory_space=pltpu.VMEM)
        specs.append(near_spec if arg.space is pltpu.VMEM else pl.BlockSpec())
    held += [arg if isinstance(arg, Held) else Held(arg, pltpu.HBM) for arg in raw]
    specs += [pl.BlockSpec(memory_space=pl.ANY)] * len(raw)
    operands = [
        arg.value
        if INTERPRET or arg.space is None
        else pltpu.with_memory_space_constraint(arg.value, arg.space)
        for arg in held
    ]
    return build(kernel, outs, operands, specs, scratch, final)


def build(kernel, outs, operands, specs, scratch, final):
    return pl.pallas_call(
        kernel,
        out_shape=[
            jax.ShapeDtypeStruct(shape, dtype)
            if INTERPRET
            else (pltpu.HBM if place in final else pltpu.VMEM)(shape, dtype)
            for place, (shape, dtype) in enumerate(outs)
        ],
        in_specs=specs,
        out_specs=[
            pl.BlockSpec() if place in final else pl.BlockSpec(memory_space=pltpu.VMEM)
            for place in range(len(outs))
        ],
        scratch_shapes=list(scratch),
        compiler_params=pltpu.CompilerParams(vmem_limit_bytes=VMEM_LIMIT),
        interpret=INTERPRET,
    )(*operands)


def round_up(n, k):
    return (n + k - 1) // k * k


def iota(shape, dim):
    return lax.broadcasted_iota(jnp.int32, shape, dim)


def gelu_terms(win, x):
    pre = dg(win, x, 0, 0)
    square = pre * pre
    tanh = jnp.tanh(pre * (GELU_C + (GELU_C * GELU_A) * square))
    return pre, square, tanh


def pool_kernel(blocks, x_ref, win_ref, wout_ref, anchor_ref, id_ref, send_ref, hsum_ref):
    width, points = x_ref.shape
    size = points // blocks
    hid = win_ref.shape[1]
    owners, rows, _ = send_ref.shape
    win = win_ref[...]
    step = 2 if blocks % 2 == 0 else 1
    hsum = jnp.zeros((hid, round_up(blocks, 8)), F32)
    for first in range(0, blocks, step):
        pre, _, tanh = gelu_terms(win, x_ref[:, pl.ds(first * size, step * size)])
        half = 0.5 * pre
        hidden = (half + half * tanh).astype(BF)
        shape = (step * size, hsum.shape[1])
        pick = (iota(shape, 1) == first + iota(shape, 0) // size).astype(F32).astype(BF)
        hsum = hsum + dg(hidden, pick, 1, 0)
    hsum = hsum.T
    hsum_ref[...] = hsum
    high, low = split_bf(hsum)
    wout = wout_ref[...]
    sums = dg(high, wout, 1, 1) + dg(low, wout, 1, 1)
    ids = id_ref[...]
    digits = jnp.concatenate([ids % DIGIT, ids // DIGIT], axis=0).astype(F32)
    packed = jnp.zeros((rows, 2 * width), F32)
    packed = jnp.concatenate(
        [
            jnp.concatenate(
                [anchor_ref[...].astype(F32)]
                + ([jnp.zeros((rows - anchor_ref.shape[0], width), F32)] if rows > anchor_ref.shape[0] else []),
                axis=0,
            ),
            jnp.concatenate(
                [
                    sums[:blocks],
                    jnp.concatenate([digits, jnp.zeros((2, width - blocks), F32)], axis=1),
                    jnp.zeros((rows - blocks - 2, width), F32),
                ],
                axis=0,
            ),
        ],
        axis=1,
    ).astype(BF)
    for owner in range(owners):
        send_ref[owner] = packed


def query_kernel(
    blocks, x_ref, g_ref, wq_ref, wp_ref, wk_ref, wv_ref, gain_ref, xp_ref, win_ref,
    q_ref, dmix_ref, wk_out, wv_out, gain_out, x_out, g_out, wp_out, slope_ref,
):
    x_out[...] = x_ref[...]
    g_out[...] = g_ref[...]
    wp_out[...] = wp_ref[...]
    wk_out[...] = wk_ref[...]
    wv_out[...] = wv_ref[...]
    gain_out[...] = gain_ref[...]
    q_ref[...] = dg(wq_ref[...], x_ref[...], 0, 0).astype(BF)
    dmix_ref[...] = dg(wp_ref[...], g_ref[...], 1, 0).astype(BF)
    win = win_ref[...]
    points = xp_ref.shape[1]
    step = points // blocks * (2 if blocks % 2 == 0 else 1)
    for first in range(0, points, step):
        pre, square, tanh = gelu_terms(win, xp_ref[:, pl.ds(first, step)])
        half = 0.5 + 0.5 * tanh
        slope = half + pre * ((half * (1.0 - tanh)) * (GELU_C + (3.0 * GELU_C * GELU_A) * square))
        slope_ref[:, pl.ds(first, step)] = slope.astype(BF)


def attend_kernel(
    blocks, size, per_owner,
    got_ref, gain_ref, wk_ref, wv_ref, q_ref, dmix_ref,
    rows_ref, normed_ref, k_ref, v_ref, p_ref, ds_ref, kt_ref, vt_ref, gain_out_ref,
):
    owners, rows, both = got_ref.shape
    width = both // 2
    total = owners * rows
    anchors = owners * per_owner
    got = got_ref[...].astype(F32)
    side = got[:, :, width:]
    sums = side.reshape(total, width)
    low = jnp.broadcast_to(side[:, blocks : blocks + 1, :], side.shape).reshape(total, width)
    high = jnp.broadcast_to(side[:, blocks + 1 : blocks + 2, :], side.shape).reshape(total, width)
    lane = iota((total, width), 1)
    place = iota((total, width), 0) % rows
    ids = jnp.sum(jnp.where(lane == place, low + high * DIGIT, 0.0), axis=1, keepdims=True)
    valid = (iota((total, 1), 0) % rows) < blocks
    ids = jnp.where(valid, ids, -1.0).astype(jnp.int32)
    member = (ids == iota((total, anchors), 1)).astype(F32).astype(BF)
    sums_bf = sums.astype(BF)
    pooled = dg(member, sums_bf, 0, 0)
    count = dg(member, jnp.ones((total, LANES), BF), 0, 0)[:, :1]
    inv_div = 1.0 / jnp.maximum(count * size, 1.0)
    anchor_rows = got[:, :per_owner, :width].reshape(anchors, width)
    asum = anchor_rows + pooled * inv_div
    inv = lax.rsqrt(jnp.mean(asum * asum, axis=1, keepdims=True) + 1e-6)
    gain = gain_ref[...]
    unit = asum * inv
    normed = (unit * gain).astype(BF)
    normed_ref[...] = normed
    keys = dg(wk_ref[...], normed, 0, 1).astype(BF)
    values = dg(wv_ref[...], normed, 0, 1).astype(BF)
    k_ref[...] = keys
    v_ref[...] = values
    depth = width // HEADS
    scale = 1.0 / depth**0.5
    for head in range(HEADS):
        part = slice(head * depth, (head + 1) * depth)
        q = q_ref[part, :]
        dmix = dmix_ref[part, :]
        scores = dg(keys[part], q, 0, 0) * scale
        top = jnp.max(scores, axis=0, keepdims=True)
        weight = jnp.exp(scores - top)
        probs = weight * (1.0 / jnp.sum(weight, axis=0, keepdims=True))
        probs_bf = probs.astype(BF)
        p_ref[head] = probs_bf
        dprobs = dg(values[part], dmix, 0, 0)
        inner = jnp.sum(probs * dprobs, axis=0, keepdims=True)
        dscore = (probs * (dprobs - inner) * scale).astype(BF)
        ds_ref[head] = dscore
        kt_ref[part, :] = dg(q, dscore, 1, 1).astype(BF)
        vt_ref[part, :] = dg(dmix, probs_bf, 1, 1).astype(BF)
    dnorm = dg(kt_ref[...], wk_ref[...], 0, 1) + dg(vt_ref[...], wv_ref[...], 0, 1)
    gain_out_ref[...] = jnp.sum(dnorm * unit, axis=0, keepdims=True)
    scaled = dnorm * gain
    dsum = inv * scaled - asum * (inv * inv * inv) * jnp.mean(scaled * asum, axis=1, keepdims=True)
    dpool = (dsum * inv_div).astype(BF)
    rows_ref[...] = dg(member, dpool, 1, 0).astype(BF).reshape(owners, rows, width)


def put_rows(ref, chunk, start, value):
    done = 0
    while done < value.shape[0]:
        index, offset = divmod(start + done, chunk)
        take = min(chunk - offset, value.shape[0] - done)
        ref[index, offset : offset + take, :] = value[done : done + take]
        done += take


def get_rows(read, chunk, start, count):
    pieces = []
    done = 0
    while done < count:
        index, offset = divmod(start + done, chunk)
        take = min(chunk - offset, count - done)
        pieces.append(read(index, offset, take))
        done += take
    return pieces[0] if len(pieces) == 1 else jnp.concatenate(pieces, axis=0)


def pack_square(ref, chunk, mats, start):
    width = mats[0].shape[0]
    for mat in mats:
        put_rows(ref, chunk, start, mat[:, :LANES])
        start += width
    for first in range(0, len(mats), 2):
        pair = jnp.concatenate([mats[first][:, LANES:], mats[first + 1][:, LANES:]], axis=1)
        put_rows(ref, chunk, start, pair)
        start += width
    return start


def swap_halves(head_ref, scratch, keep_ref, send_ref):
    half = keep_ref.shape[0]
    head = head_ref[0]
    keep_ref[...] = scratch[pl.ds(head * half, half)].astype(keep_ref.dtype)
    send_ref[...] = scratch[pl.ds((1 - head) * half, half)].astype(send_ref.dtype)


def fetch_kernel(*refs):
    *refs, sems = refs
    count = len(refs) // 2
    sources, (both, *rest) = refs[:count], refs[count + 1 :]
    points = sources[0].shape[1]
    targets = [both.at[:, :points], both.at[:, points:]] + rest
    copies = [
        pltpu.make_async_copy(source, target, sems.at[place])
        for place, (source, target) in enumerate(zip(sources, targets))
    ]
    for copy in copies:
        copy.start()
    for copy in copies:
        copy.wait()


def finish_kernel(
    chunk, head_ref, p_ref, ds_ref, k_ref, v_ref, kt_ref, vt_ref, normed_ref, gain_ref, x_ref, g_ref,
    wp_ref, out_ref, keep_ref, send_ref, mixed_ref, dq_ref, pack_ref,
):
    width = k_ref.shape[0]
    depth = width // HEADS
    for head in range(HEADS):
        part = slice(head * depth, (head + 1) * depth)
        mixed_ref[part, :] = dg(v_ref[part, :], p_ref[head], 1, 0).astype(BF)
        dq_ref[part, :] = dg(k_ref[part, :], ds_ref[head], 1, 0).astype(BF)
    mixed = mixed_ref[...]
    out_ref[...] = dg(wp_ref[...], mixed, 0, 0).astype(BF)
    mats = [
        dg(x_ref[...], dq_ref[...], 1, 1),
        dg(normed_ref[...], kt_ref[...], 0, 1),
        dg(normed_ref[...], vt_ref[...], 0, 1),
        dg(mixed, g_ref[...], 1, 1),
    ]
    pieces, rows, _ = pack_ref.shape
    pack_square(pack_ref, chunk, mats, 0)
    gain = gain_ref[...]
    pack_ref[:, chunk:, :] = jnp.zeros((pieces, rows - chunk, LANES), F32)
    pack_ref[0, chunk : chunk + 1, :] = gain[:, :LANES]
    rest = width - LANES
    pack_ref[0, chunk + 1 : chunk + 2, :] = jnp.concatenate(
        [gain[:, LANES:], jnp.zeros((1, LANES - rest), F32)], axis=1
    )
    swap_halves(head_ref, pack_ref, keep_ref, send_ref)


def back_kernel(
    blocks, chunk, head_ref, got_ref, both_ref, slope_ref, hsum_ref, *refs,
):
    dpre_ref, keep_ref, send_ref, pack_ref = refs[-4:]
    width = both_ref.shape[0]
    points = slope_ref.shape[1]
    size = points // blocks
    x_ref = both_ref.at[:, :points]
    wout_ref = both_ref.at[:, points:]
    grad = jnp.sum(got_ref[...].astype(F32), axis=0)[: hsum_ref.shape[0]].astype(BF)
    dhid = dg(wout_ref[...], grad, 0, 1)
    for block in range(blocks):
        cols = pl.ds(block * size, size)
        dpre_ref[:, cols] = (slope_ref[:, cols].astype(F32) * dhid[:, block : block + 1]).astype(BF)
    gin = dg(x_ref[...], dpre_ref[...], 1, 1)
    high, low = split_bf(hsum_ref[...])
    gout = dg(grad, high, 0, 0) + dg(grad, low, 0, 0)
    start = 0
    for mat in (gin, gout):
        for lane in range(0, mat.shape[1], LANES):
            put_rows(pack_ref, chunk, start, mat[:, lane : lane + LANES])
            start += width
    swap_halves(head_ref, pack_ref, keep_ref, send_ref)


def point_grad_kernel(win_ref, dpre_ref, after_ref, out_ref):
    out_ref[...] = dg(win_ref[...], dpre_ref[...], 1, 0).astype(BF)


def design_kernel(shares, share_ref, keep_ref, got_ref, *refs):
    total_ref = refs[-1]
    total = keep_ref[...].astype(F32) + got_ref[...].astype(F32)
    total_ref[...] = total.reshape(total_ref.shape)
    for shift in range(shares):
        share = lax.rem(share_ref[0] + shift, shares)
        refs[shift][...] = total_ref[:, pl.ds(share, 1)][:, 0].astype(BF)


def join_kernel(shares, *refs):
    _, out_ref = refs[-2:]
    ka_ref, kp_ref, rp_ref = refs[:3]
    total = ka_ref[...].astype(F32)
    for ref in refs[3:-2]:
        total = total + ref[...].astype(F32)
    groups, rows, _ = total.shape
    part = rows // shares
    total = total.astype(BF)
    for group in range(groups):
        for share in range(shares):
            out_ref[group * shares + share, :part, :] = total[group, share * part : (share + 1) * part]
    out_ref[:, part:, :] = (kp_ref[...].astype(F32) + rp_ref[...].astype(F32)).astype(BF)


def sum_kernel(shares, part, got_ref, out_ref):
    peers = out_ref.shape[0]
    for share in range(shares):
        total = got_ref[share, :part, :].astype(F32)
        for peer in range(share + shares, peers, shares):
            total = total + got_ref[peer, :part, :].astype(F32)
        total = total.astype(BF)
        for peer in range(peers):
            out_ref[peer, share * part : (share + 1) * part, :] = total
    total = jnp.sum(got_ref[:, part:, :].astype(F32), axis=0).astype(BF)
    for peer in range(peers):
        out_ref[peer, shares * part :, :] = total


def unpack_kernel(
    shares, chunk_a, rows_a, chunk_p, head_ref, mine_ref, other_ref,
    gin_ref, gout_ref, gq_ref, gk_ref, gv_ref, gp_ref, gain_ref, all_ref,
):
    peers = mine_ref.shape[0]
    head = head_ref[0]
    all_ref[pl.ds(head * peers, peers)] = mine_ref[...]
    all_ref[pl.ds((1 - head) * peers, peers)] = other_ref[...]
    part = rows_a // shares

    def read_a(index, offset, take):
        group, share = divmod(index, shares)

        def read(source, start, count):
            row = share * part + start
            return all_ref[group * shares + source, row : row + count, :].astype(F32)

        return get_rows(read, part, offset, take)

    def read_p(index, offset, take):
        return all_ref[index, rows_a + offset : rows_a + offset + take, :].astype(F32)

    width = gq_ref.shape[0]
    squares = (gq_ref, gk_ref, gv_ref, gp_ref)
    start = 0
    for ref in squares:
        ref[:, :LANES] = get_rows(read_a, chunk_a, start, width)
        start += width
    rest = width - LANES
    for first in range(0, len(squares), 2):
        pair = get_rows(read_a, chunk_a, start, width)
        squares[first][:, LANES:] = pair[:, :rest]
        squares[first + 1][:, LANES:] = pair[:, rest:]
        start += width
    tail = read_a(0, chunk_a, 2)
    gain_ref[...] = jnp.concatenate([tail[:1], tail[1:2, :rest]], axis=1)
    start = 0
    for ref in (gin_ref, gout_ref):
        for lane in range(0, ref.shape[1], LANES):
            ref[:, lane : lane + LANES] = get_rows(read_p, chunk_p, start, width)
            start += width


def on_device(
    point_feats, block_anchor, anchor_feats, query_feats, out_grad, norm_gain,
    w_in, w_out, w_query, w_key, w_value, w_proj,
):
    team = ("geom", "head")
    crowd = ("geom", "design")
    owners = lax.axis_size(team)
    peers = lax.axis_size(crowd)
    xt = point_feats[0].T
    qt = query_feats[0].T
    gt = out_grad[0].T
    wot = w_out.T
    blocks = block_anchor.shape[1]
    per_owner, width = anchor_feats.shape[1:]
    points = xt.shape[1]
    queries = qt.shape[1]
    hid = w_in.shape[1]
    size = points // blocks
    anchors = owners * per_owner
    rows = round_up(max(per_owner, blocks + 2), 16)
    shares = lax.axis_size("design")
    head = lax.axis_index("head").astype(jnp.int32).reshape(1)
    share = lax.axis_index("design").astype(jnp.int32).reshape(1)
    pieces = 2 * peers
    chunk_a = 6 * width // pieces
    rows_a = round_up(chunk_a + 2, 8 * shares)
    chunk_p = 2 * width * hid // LANES // pieces

    send, hsum = call(
        functools.partial(pool_kernel, blocks),
        [((owners, rows, 2 * width), BF), ((round_up(blocks, 8), hid), F32)],
        xt, w_in, wot, anchor_feats[0], block_anchor,
        final=(1,),
    )
    got = lax.all_to_all(send, team, 0, 0, tiled=True)
    qp, dmix, wk, wv, gain_row, qn, gn, wpn, slope = call(
        functools.partial(query_kernel, blocks),
        [
            ((width, queries), BF),
            ((width, queries), BF),
            ((width, width), BF),
            ((width, width), BF),
            ((1, width), F32),
            ((width, queries), BF),
            ((width, queries), BF),
            ((width, width), BF),
            ((hid, points), BF),
        ],
        qt, gt, w_query, w_proj, w_key, w_value, norm_gain.reshape(1, width), xt, w_in,
        final=(8,),
    )
    pair_shape = (HEADS, anchors, queries)
    rows_out, normed, keys, values, probs, dscore, kt, vt, gain_part = call(
        functools.partial(attend_kernel, blocks, size, per_owner),
        [
            ((owners, rows, width), BF),
            ((anchors, width), BF),
            ((width, anchors), BF),
            ((width, anchors), BF),
            (pair_shape, BF),
            (pair_shape, BF),
            ((width, anchors), BF),
            ((width, anchors), BF),
            ((1, width), F32),
        ],
        *near(got, gain_row, wk, wv, qp, dmix),
    )
    back = lax.all_to_all(rows_out, team, 0, 0, tiled=True)
    shape_a = ((peers, rows_a, LANES), BF)
    attended, keep_a, send_a = call(
        functools.partial(finish_kernel, chunk_a),
        [((width, queries), BF), shape_a, shape_a],
        head, *near(probs, dscore, keys, values, kt, vt, normed, gain_part, qn, gn, wpn),
        scratch=[
            pltpu.VMEM((width, queries), BF),
            pltpu.VMEM((width, queries), BF),
            pltpu.VMEM((pieces, rows_a, LANES), F32),
        ],
        smem=1,
        final=(0,),
    )
    both, slope, hsum, win = call(
        fetch_kernel,
        [((width, points + hid), BF), ((hid, points), BF), (hsum.shape, F32), ((width, hid), BF)],
        scratch=[pltpu.SemaphoreType.DMA((5,))],
        raw=(xt, wot, slope, hsum, w_in) + near(send_a),
    )
    swap = [(0, 1), (1, 0)]
    shape_p = ((peers, chunk_p, LANES), BF)
    recv_a = lax.ppermute(send_a, "head", swap)
    groups = peers // shares
    shape_d = ((groups, rows_a, LANES), BF)
    keep_d, *sends_d = call(
        functools.partial(design_kernel, shares),
        [shape_d] * shares,
        share, *near(keep_a, recv_a),
        scratch=[pltpu.VMEM((groups, shares, rows_a, LANES), F32)],
        smem=1,
    )
    recvs_d = [
        lax.ppermute(send, "design", [(i, (i + shift) % shares) for i in range(shares)])
        for shift, send in enumerate(sends_d, 1)
    ]
    dpre, keep_p, send_p = call(
        functools.partial(back_kernel, blocks, chunk_p),
        [((hid, points), BF), shape_p, shape_p],
        head, *near(back, both, slope, hsum),
        scratch=[pltpu.VMEM((pieces, chunk_p, LANES), F32)],
        smem=1,
        raw=near(keep_d),
    )
    recv_p = lax.ppermute(send_p, "head", swap)
    (point_grad,) = call(
        point_grad_kernel, [((width, points), BF)], *near(win, dpre), final=(0,), raw=near(send_p)
    )
    (joined,) = call(
        functools.partial(join_kernel, shares),
        [((peers, rows_a // shares + chunk_p, LANES), BF)],
        *near(keep_d, keep_p, recv_p, *recvs_d), raw=(point_grad,),
    )
    scattered = lax.all_to_all(joined, crowd, 0, 0, tiled=True)
    (summed,) = call(
        functools.partial(sum_kernel, shares, rows_a // shares),
        [((peers, rows_a + chunk_p, LANES), BF)],
        *near(scattered),
    )
    mine = lax.all_to_all(summed, crowd, 0, 0, tiled=True)
    other = lax.ppermute(mine, "head", swap)
    square = ((width, width), F32)
    gin, gout, gq, gk, gv, gp, gain = call(
        functools.partial(unpack_kernel, shares, chunk_a, rows_a, chunk_p),
        [((width, hid), F32), ((width, hid), F32), square, square, square, square, ((1, width), F32)],
        head, *near(mine, other),
        scratch=[pltpu.VMEM((pieces, rows_a + chunk_p, LANES), BF)],
        smem=1,
        final=range(7),
    )
    return (
        attended.T[None], point_grad.T[None], gin, gout.T, gq, gk, gv, gp, gain.reshape(width),
    )


def solution(mesh):
    split = P(("groups", "design"), ("geom", "head"), None)
    placed = (split, P(("groups", "design"), ("geom", "head")), split, split, split) + (P(),) * 7
    grads = (P("groups", None),) * 6 + (P("groups"),)

    return jax.shard_map(
        on_device, mesh=mesh, in_specs=placed, out_specs=(split, split) + grads, check_vma=False
    )
```

```python
import functools

import jax
import jax.numpy as jnp
from jax import lax
from jax.experimental import pallas as pl
from jax.experimental.pallas import tpu as pltpu
from jax.sharding import PartitionSpec as P


HEADS = 3
LANES = 128
DIGIT = 128
INTERPRET = False
VMEM_LIMIT = 24 << 20
BF = jnp.bfloat16
F32 = jnp.float32
GELU_C = 0.7978845608028654
GELU_A = 0.044715


def dg(a, b, ca, cb):
    return lax.dot_general(a, b, (((ca,), (cb,)), ((), ())), preferred_element_type=F32)


def split_bf(x):
    high = x.astype(BF)
    return high, (x - high.astype(F32)).astype(BF)


class Held:
    def __init__(self, value, space):
        self.value, self.space = value, space


def near(*values):
    return tuple(Held(value, pltpu.VMEM) for value in values)


def call(kernel, outs, *args, scratch=(), smem=0, final=(), raw=(), update=False):
    held = [Held(arg, None) for arg in args[:smem]]
    held += [arg if isinstance(arg, Held) else Held(arg, pltpu.HBM) for arg in args[smem:]]
    specs = [pl.BlockSpec(memory_space=pltpu.SMEM)] * smem
    for arg in held[smem:]:
        near_spec = pl.BlockSpec(memory_space=pltpu.VMEM)
        specs.append(near_spec if arg.space is pltpu.VMEM else pl.BlockSpec())
    held += [arg if isinstance(arg, Held) else Held(arg, pltpu.HBM) for arg in raw]
    specs += [pl.BlockSpec(memory_space=pl.ANY)] * len(raw)
    operands = [
        arg.value
        if INTERPRET or arg.space is None
        else pltpu.with_memory_space_constraint(arg.value, arg.space)
        for arg in held
    ]
    if update:
        aliases = {len(operands) - len(raw) + place: place for place in range(len(raw))}
        return build(kernel, outs, operands, specs, scratch, range(len(outs)), aliases, pl.ANY)
    return build(kernel, outs, operands, specs, scratch, final)


def build(kernel, outs, operands, specs, scratch, final, aliases=None, space=None):
    return pl.pallas_call(
        kernel,
        out_shape=[
            jax.ShapeDtypeStruct(shape, dtype)
            if INTERPRET
            else (pltpu.HBM if place in final else pltpu.VMEM)(shape, dtype)
            for place, (shape, dtype) in enumerate(outs)
        ],
        in_specs=specs,
        out_specs=[
            pl.BlockSpec(memory_space=space if place in final else pltpu.VMEM)
            for place in range(len(outs))
        ],
        scratch_shapes=list(scratch),
        compiler_params=pltpu.CompilerParams(vmem_limit_bytes=VMEM_LIMIT),
        input_output_aliases=aliases or {},
        interpret=INTERPRET,
    )(*operands)


def round_up(n, k):
    return (n + k - 1) // k * k


def iota(shape, dim):
    return lax.broadcasted_iota(jnp.int32, shape, dim)


def gelu_terms(win, x):
    pre = dg(win, x, 0, 0)
    square = pre * pre
    tanh = jnp.tanh(pre * (GELU_C + (GELU_C * GELU_A) * square))
    return pre, square, tanh


def pool_kernel(blocks, x_ref, win_ref, wout_ref, anchor_ref, id_ref, send_ref, hsum_ref):
    width, points = x_ref.shape
    size = points // blocks
    hid = win_ref.shape[1]
    owners, rows, _ = send_ref.shape
    win = win_ref[...]
    step = 2 if blocks % 2 == 0 else 1
    hsum = jnp.zeros((hid, round_up(blocks, 8)), F32)
    for first in range(0, blocks, step):
        pre, _, tanh = gelu_terms(win, x_ref[:, pl.ds(first * size, step * size)])
        half = 0.5 * pre
        hidden = (half + half * tanh).astype(BF)
        shape = (step * size, hsum.shape[1])
        pick = (iota(shape, 1) == first + iota(shape, 0) // size).astype(F32).astype(BF)
        hsum = hsum + dg(hidden, pick, 1, 0)
    hsum = hsum.T
    hsum_ref[...] = hsum
    high, low = split_bf(hsum)
    wout = wout_ref[...]
    sums = dg(jnp.concatenate([high, low], axis=0), wout, 1, 1)
    sums = sums[: hsum.shape[0]] + sums[hsum.shape[0] :]
    ids = id_ref[...]
    digits = jnp.concatenate([ids % DIGIT, ids // DIGIT], axis=0).astype(F32)
    packed = jnp.zeros((rows, 2 * width), F32)
    packed = jnp.concatenate(
        [
            jnp.concatenate(
                [anchor_ref[...].astype(F32)]
                + ([jnp.zeros((rows - anchor_ref.shape[0], width), F32)] if rows > anchor_ref.shape[0] else []),
                axis=0,
            ),
            jnp.concatenate(
                [
                    sums[:blocks],
                    jnp.concatenate([digits, jnp.zeros((2, width - blocks), F32)], axis=1),
                    jnp.zeros((rows - blocks - 2, width), F32),
                ],
                axis=0,
            ),
        ],
        axis=1,
    ).astype(BF)
    for owner in range(owners):
        send_ref[owner] = packed


def query_kernel(
    blocks, x_ref, g_ref, wq_ref, wp_ref, wk_ref, wv_ref, gain_ref, xp_ref, win_ref,
    q_ref, dmix_ref, wk_out, wv_out, gain_out, x_out, g_out, wp_out, slope_ref,
):
    x_out[...] = x_ref[...]
    g_out[...] = g_ref[...]
    wp_out[...] = wp_ref[...]
    wk_out[...] = wk_ref[...]
    wv_out[...] = wv_ref[...]
    gain_out[...] = gain_ref[...]
    q_ref[...] = dg(wq_ref[...], x_ref[...], 0, 0).astype(BF)
    dmix_ref[...] = dg(wp_ref[...], g_ref[...], 1, 0).astype(BF)
    win = win_ref[...]
    points = xp_ref.shape[1]
    step = points // blocks * (2 if blocks % 2 == 0 else 1)
    for first in range(0, points, step):
        pre, square, tanh = gelu_terms(win, xp_ref[:, pl.ds(first, step)])
        half = 0.5 + 0.5 * tanh
        slope = half + pre * ((half * (1.0 - tanh)) * (GELU_C + (3.0 * GELU_C * GELU_A) * square))
        slope_ref[:, pl.ds(first, step)] = slope.astype(BF)


def attend_kernel(
    blocks, size, per_owner,
    got_ref, gain_ref, wk_ref, wv_ref, q_ref, dmix_ref,
    rows_ref, normed_ref, k_ref, v_ref, p_ref, ds_ref, kt_ref, vt_ref,
):
    owners, rows, both = got_ref.shape
    width = both // 2
    total = owners * rows
    anchors = owners * per_owner
    got = got_ref[...].astype(F32)
    side = got[:, :, width:]
    sums = side.reshape(total, width)
    low = jnp.broadcast_to(side[:, blocks : blocks + 1, :], side.shape).reshape(total, width)
    high = jnp.broadcast_to(side[:, blocks + 1 : blocks + 2, :], side.shape).reshape(total, width)
    lane = iota((total, width), 1)
    place = iota((total, width), 0) % rows
    ids = jnp.sum(jnp.where(lane == place, low + high * DIGIT, 0.0), axis=1, keepdims=True)
    valid = (iota((total, 1), 0) % rows) < blocks
    ids = jnp.where(valid, ids, -1.0).astype(jnp.int32)
    member = (ids == iota((total, anchors), 1)).astype(F32).astype(BF)
    sums_bf = sums.astype(BF)
    pooled = dg(member, sums_bf, 0, 0)
    count = dg(member, jnp.ones((total, LANES), BF), 0, 0)[:, :1]
    inv_div = 1.0 / jnp.maximum(count * size, 1.0)
    anchor_rows = got[:, :per_owner, :width].reshape(anchors, width)
    asum = anchor_rows + pooled * inv_div
    inv = lax.rsqrt(jnp.mean(asum * asum, axis=1, keepdims=True) + 1e-6)
    gain = gain_ref[...]
    unit = asum * inv
    normed = (unit * gain).astype(BF)
    normed_ref[...] = normed
    keys = dg(normed, wk_ref[...], 1, 0).astype(BF)
    values = dg(normed, wv_ref[...], 1, 0).astype(BF)
    k_ref[...] = keys
    v_ref[...] = values
    depth = width // HEADS
    scale = 1.0 / depth**0.5
    key_parts, value_parts = [], []
    for head in range(HEADS):
        part = slice(head * depth, (head + 1) * depth)
        q = q_ref[part, :]
        dmix = dmix_ref[part, :]
        scores = dg(keys[:, part], q, 1, 0) * scale
        top = jnp.max(scores, axis=0, keepdims=True)
        weight = jnp.exp(scores - top)
        probs = weight * (1.0 / jnp.sum(weight, axis=0, keepdims=True))
        probs_bf = probs.astype(BF)
        p_ref[head] = probs_bf
        dprobs = dg(values[:, part], dmix, 1, 0)
        inner = jnp.sum(probs * dprobs, axis=0, keepdims=True)
        dscore = (probs * (dprobs - inner) * scale).astype(BF)
        ds_ref[head] = dscore
        key_parts.append(dg(dscore, q, 1, 1))
        value_parts.append(dg(probs_bf, dmix, 1, 1))
    kt = jnp.concatenate(key_parts, axis=1).astype(BF)
    vt = jnp.concatenate(value_parts, axis=1).astype(BF)
    kt_ref[...] = kt
    vt_ref[...] = vt
    dnorm = dg(kt, wk_ref[...], 1, 1) + dg(vt, wv_ref[...], 1, 1)
    dgain = jnp.sum(dnorm * unit, axis=0, keepdims=True)
    scaled = dnorm * gain
    dsum = inv * scaled - asum * (inv * inv * inv) * jnp.mean(scaled * asum, axis=1, keepdims=True)
    dpool = (dsum * inv_div).astype(BF)
    spare = iota((total, 1), 0) % rows == blocks
    picked = jnp.where(spare, dgain, dg(member, dpool, 1, 0))
    picked = picked.reshape(owners, rows, width)
    rest = picked[:, :, LANES:]
    rest = jnp.concatenate([rest[:, : rows // 2], rest[:, rows // 2 :]], axis=2)
    rows_ref[...] = jnp.concatenate([picked[:, :, :LANES], rest], axis=1).astype(BF)


def put_rows(ref, chunk, start, value):
    done = 0
    while done < value.shape[0]:
        index, offset = divmod(start + done, chunk)
        take = min(chunk - offset, value.shape[0] - done)
        ref[index, offset : offset + take, :] = value[done : done + take]
        done += take


def get_rows(read, chunk, start, count):
    pieces = []
    done = 0
    while done < count:
        index, offset = divmod(start + done, chunk)
        take = min(chunk - offset, count - done)
        pieces.append(read(index, offset, take))
        done += take
    return pieces[0] if len(pieces) == 1 else jnp.concatenate(pieces, axis=0)


def pack_square(ref, chunk, mats):
    width = mats[0].shape[0]
    start = 0
    for first in range(0, len(mats), 2):
        left, right = mats[first : first + 2]
        pair = jnp.concatenate([left[:, LANES:], right[:, LANES:]], axis=1)
        for slot in (left[:, :LANES], right[:, :LANES], pair):
            put_rows(ref, chunk, start, slot)
            start += width


def swap_halves(head_ref, scratch, keep_ref, send_ref):
    half = keep_ref.shape[0]
    head = head_ref[0]
    keep_ref[...] = scratch[pl.ds(head * half, half)].astype(keep_ref.dtype)
    send_ref[...] = scratch[pl.ds((1 - head) * half, half)].astype(send_ref.dtype)


def fetch_kernel(*refs):
    *refs, sems = refs
    count = len(refs) // 2
    sources, (both, *rest) = refs[:count], refs[count + 1 :]
    points = sources[0].shape[1]
    targets = [both.at[:, :points], both.at[:, points:]] + rest
    copies = [
        pltpu.make_async_copy(source, target, sems.at[place])
        for place, (source, target) in enumerate(zip(sources, targets))
    ]
    for copy in copies:
        copy.start()
    for copy in copies:
        copy.wait()


def finish_kernel(
    chunk, head_ref, p_ref, ds_ref, k_ref, v_ref, kt_ref, vt_ref, normed_ref, x_ref, g_ref,
    wp_ref, out_ref, keep_ref, send_ref, mixed_ref, dq_ref, pack_ref,
):
    width = k_ref.shape[1]
    depth = width // HEADS
    for head in range(HEADS):
        part = slice(head * depth, (head + 1) * depth)
        mixed_ref[part, :] = dg(v_ref[:, part], p_ref[head], 0, 0).astype(BF)
        dq_ref[part, :] = dg(k_ref[:, part], ds_ref[head], 0, 0).astype(BF)
    mixed = mixed_ref[...]
    out_ref[...] = dg(wp_ref[...], mixed, 0, 0).astype(BF)
    mats = [
        dg(x_ref[...], dq_ref[...], 1, 1),
        dg(normed_ref[...], kt_ref[...], 0, 0),
        dg(normed_ref[...], vt_ref[...], 0, 0),
        dg(mixed, g_ref[...], 1, 1),
    ]
    if pack_ref.shape[1] > chunk:
        pack_ref[:, chunk:, :] = jnp.zeros((pack_ref.shape[0], pack_ref.shape[1] - chunk, LANES), F32)
    pack_square(pack_ref, chunk, mats)
    swap_halves(head_ref, pack_ref, keep_ref, send_ref)


def back_kernel(
    blocks, chunk, head_ref, got_ref, both_ref, slope_ref, hsum_ref, *refs,
):
    dpre_ref, keep_ref, send_ref, gain_ref, pack_ref = refs[-5:]
    width = both_ref.shape[0]
    points = slope_ref.shape[1]
    size = points // blocks
    x_ref = both_ref.at[:, :points]
    wout_ref = both_ref.at[:, points:]
    total = jnp.sum(got_ref[...].astype(F32), axis=0)
    rows = total.shape[0] * 2 // 3
    rest = total[rows:]
    rest = jnp.concatenate([rest[:, : width - LANES], rest[:, width - LANES :]], axis=0)
    total = jnp.concatenate([total[:rows], rest], axis=1)
    gain_ref[...] = total[blocks : blocks + 1]
    grad = total[: hsum_ref.shape[0]].astype(BF)
    dhid = dg(wout_ref[...], grad, 0, 1)
    for block in range(blocks):
        cols = pl.ds(block * size, size)
        dpre_ref[:, cols] = (slope_ref[:, cols].astype(F32) * dhid[:, block : block + 1]).astype(BF)
    gin = dg(x_ref[...], dpre_ref[...], 1, 1)
    high, low = split_bf(hsum_ref[...])
    gout = dg(grad, high, 0, 0) + dg(grad, low, 0, 0)
    start = 0
    for mat in (gin, gout):
        for lane in range(0, mat.shape[1], LANES):
            put_rows(pack_ref, chunk, start, mat[:, lane : lane + LANES])
            start += width
    swap_halves(head_ref, pack_ref, keep_ref, send_ref)


def point_grad_kernel(win_ref, dpre_ref, after_ref, out_ref):
    out_ref[...] = dg(win_ref[...], dpre_ref[...], 1, 0).astype(BF)


def design_kernel(shares, share_ref, keep_ref, got_ref, *refs):
    total_ref = refs[-1]
    total = keep_ref[...].astype(F32) + got_ref[...].astype(F32)
    total_ref[...] = total.reshape(total_ref.shape)
    for shift in range(shares):
        share = lax.rem(share_ref[0] + shift, shares)
        refs[shift][...] = total_ref[:, pl.ds(share, 1)][:, 0].astype(BF)


def join_kernel(shares, part, *refs):
    out_ref = refs[-1]
    ka_ref, kp_ref, rp_ref, gain_ref = refs[:4]
    total = ka_ref[...].astype(F32)
    for ref in refs[4:-2]:
        total = total + ref[...].astype(F32)
    groups = total.shape[0]
    top = out_ref.shape[1] - kp_ref.shape[1]
    gain = gain_ref[...] * (1.0 / groups)
    width = gain.shape[1]
    tail = [gain[:, :LANES], jnp.concatenate([gain[:, LANES:], jnp.zeros((1, 2 * LANES - width), F32)], axis=1)]
    tail = jnp.concatenate(tail + [jnp.zeros((top - part - 2, LANES), F32)], axis=0)
    for group in range(groups):
        for share in range(shares):
            piece = total[group, share * part : (share + 1) * part]
            out_ref[group * shares + share, :top, :] = jnp.concatenate([piece, tail], axis=0).astype(BF)
    out_ref[:, top:, :] = (kp_ref[...].astype(F32) + rp_ref[...].astype(F32)).astype(BF)


def sum_kernel(shares, part, top, got_ref, out_ref, gain_ref):
    peers = out_ref.shape[0]
    gain = None
    for share in range(shares):
        total = got_ref[share, :top, :].astype(F32)
        for peer in range(share + shares, peers, shares):
            total = total + got_ref[peer, :top, :].astype(F32)
        tail = total[part : part + 2]
        gain = tail if gain is None else gain + tail
        total = total[:part].astype(BF)
        for peer in range(peers):
            out_ref[peer, share * part : (share + 1) * part, :] = total
    width = gain_ref.shape[1]
    gain_ref[...] = jnp.concatenate([gain[:1], gain[1:2, : width - LANES]], axis=1)
    total = jnp.sum(got_ref[:, top:, :].astype(F32), axis=0).astype(BF)
    for peer in range(peers):
        out_ref[peer, shares * part :, :] = total


def unpack_kernel(shares, part, chunk_a, chunk_p, flip, head_ref, half_ref, gain_ref, *refs):
    left_ref, right_ref, wide_ref, sems = refs[-4:]
    targets = refs[-11:-5]
    gain_out = refs[-5]
    width = left_ref.shape[0]
    rows_a = shares * part

    def read_a(index, offset, take):
        group, share = divmod(index, shares)

        def read(source, start, count):
            row = share * part + start
            return half_ref[group * shares + source, row : row + count, :].astype(F32)

        return get_rows(read, part, offset, take)

    def read_p(index, offset, take):
        return half_ref[index, rows_a + offset : rows_a + offset + take, :].astype(F32)

    for slot in range(wide_ref.shape[1] // LANES):
        wide_ref[:, slot * LANES : (slot + 1) * LANES] = get_rows(read_p, chunk_p, slot * width, width)
    left_ref[:, :LANES] = get_rows(read_a, chunk_a, 0, width)
    right_ref[:, :LANES] = get_rows(read_a, chunk_a, width, width)
    pair = get_rows(read_a, chunk_a, 2 * width, width)
    rest = width - LANES
    left_ref[:, LANES:] = pair[:, :rest]
    right_ref[:, LANES:] = pair[:, rest:]
    if not flip:
        extra = pltpu.make_async_copy(gain_ref, gain_out, sems.at[3])
        extra.start()
    half = 1 - head_ref[0] if flip else head_ref[0]
    for which in range(2):

        @pl.when(half == which)
        def _():
            copies = [
                pltpu.make_async_copy(source, target, sems.at[place])
                for place, (source, target) in enumerate(
                    zip((left_ref, right_ref, wide_ref), targets[3 * which : 3 * which + 3])
                )
            ]
            for copy in copies:
                copy.start()
            for copy in copies:
                copy.wait()

    if not flip:
        extra.wait()


def on_device(
    point_feats, block_anchor, anchor_feats, query_feats, out_grad, norm_gain,
    w_in, w_out, w_query, w_key, w_value, w_proj,
):
    team = ("geom", "head")
    crowd = ("geom", "design")
    owners = lax.axis_size(team)
    peers = lax.axis_size(crowd)
    xt = point_feats[0].T
    qt = query_feats[0].T
    gt = out_grad[0].T
    wot = w_out.T
    blocks = block_anchor.shape[1]
    per_owner, width = anchor_feats.shape[1:]
    points = xt.shape[1]
    queries = qt.shape[1]
    hid = w_in.shape[1]
    size = points // blocks
    anchors = owners * per_owner
    rows = round_up(max(per_owner, blocks + 2), 16)
    shares = lax.axis_size("design")
    head = lax.axis_index("head").astype(jnp.int32).reshape(1)
    share = lax.axis_index("design").astype(jnp.int32).reshape(1)
    pieces = 2 * peers
    chunk_a = 6 * width // pieces
    rows_a = round_up(chunk_a, 4 * shares)
    part = rows_a // shares
    top = round_up(part + 2, 8)
    chunk_p = 2 * width * hid // LANES // pieces

    send, hsum = call(
        functools.partial(pool_kernel, blocks),
        [((owners, rows, 2 * width), BF), ((round_up(blocks, 8), hid), F32)],
        xt, w_in, wot, anchor_feats[0], block_anchor,
    )
    got = lax.all_to_all(send, team, 0, 0, tiled=True)
    qp, dmix, wk, wv, gain_row, qn, gn, wpn, slope = call(
        functools.partial(query_kernel, blocks),
        [
            ((width, queries), BF),
            ((width, queries), BF),
            ((width, width), BF),
            ((width, width), BF),
            ((1, width), F32),
            ((width, queries), BF),
            ((width, queries), BF),
            ((width, width), BF),
            ((hid, points), BF),
        ],
        qt, gt, w_query, w_proj, w_key, w_value, norm_gain.reshape(1, width), xt, w_in,
    )
    pair_shape = (HEADS, anchors, queries)
    rows_out, normed, keys, values, probs, dscore, kt, vt = call(
        functools.partial(attend_kernel, blocks, size, per_owner),
        [
            ((owners, rows * width // LANES, LANES), BF),
            ((anchors, width), BF),
            ((anchors, width), BF),
            ((anchors, width), BF),
            (pair_shape, BF),
            (pair_shape, BF),
            ((anchors, width), BF),
            ((anchors, width), BF),
        ],
        *near(got, gain_row, wk, wv, qp, dmix),
    )
    back = lax.all_to_all(rows_out, team, 0, 0, tiled=True)
    shape_a = ((peers, rows_a, LANES), BF)
    attended, keep_a, send_a = call(
        functools.partial(finish_kernel, chunk_a),
        [((width, queries), BF), shape_a, shape_a],
        head, *near(probs, dscore, keys, values, kt, vt, normed, qn, gn, wpn),
        scratch=[
            pltpu.VMEM((width, queries), BF),
            pltpu.VMEM((width, queries), BF),
            pltpu.VMEM((pieces, rows_a, LANES), F32),
        ],
        smem=1,
        final=(0,),
    )
    both, win = call(
        fetch_kernel,
        [((width, points + hid), BF), ((width, hid), BF)],
        scratch=[pltpu.SemaphoreType.DMA((3,))],
        raw=(xt, wot, w_in) + near(send_a),
    )
    swap = [(0, 1), (1, 0)]
    shape_p = ((peers, chunk_p, LANES), BF)
    recv_a = lax.ppermute(send_a, "head", swap)
    groups = peers // shares
    shape_d = ((groups, rows_a, LANES), BF)
    keep_d, *sends_d = call(
        functools.partial(design_kernel, shares),
        [shape_d] * shares,
        share, *near(keep_a, recv_a),
        scratch=[pltpu.VMEM((groups, shares, rows_a, LANES), F32)],
        smem=1,
    )
    recvs_d = [
        lax.ppermute(send, "design", [(i, (i + shift) % shares) for i in range(shares)])
        for shift, send in enumerate(sends_d, 1)
    ]
    dpre, keep_p, send_p, dgain = call(
        functools.partial(back_kernel, blocks, chunk_p),
        [((hid, points), BF), shape_p, shape_p, ((1, width), F32)],
        head, *near(back, both, slope, hsum),
        scratch=[pltpu.VMEM((pieces, chunk_p, LANES), F32)],
        smem=1,
        raw=near(keep_d),
    )
    recv_p = lax.ppermute(send_p, "head", swap)
    (point_grad,) = call(
        point_grad_kernel, [((width, points), BF)], *near(win, dpre), final=(0,), raw=near(send_p)
    )
    (joined,) = call(
        functools.partial(join_kernel, shares, part),
        [((peers, top + chunk_p, LANES), BF)],
        *near(keep_d, keep_p, recv_p, dgain, *recvs_d), raw=(point_grad,),
    )
    scattered = lax.all_to_all(joined, crowd, 0, 0, tiled=True)
    summed, gain = call(
        functools.partial(sum_kernel, shares, part, top),
        [((peers, rows_a + chunk_p, LANES), BF), ((1, width), F32)],
        *near(scattered),
    )
    mine = lax.all_to_all(summed, crowd, 0, 0, tiled=True)
    other = lax.ppermute(mine, "head", swap)
    square, wide = ((width, width), F32), ((width, hid), F32)
    grads = ()
    for flip, half in ((False, mine), (True, other)):
        grads = call(
            functools.partial(unpack_kernel, shares, part, chunk_a, chunk_p, flip),
            [square, square, wide] * 2 + [((1, width), F32)],
            head, *near(half, gain),
            scratch=[pltpu.VMEM(*square), pltpu.VMEM(*square), pltpu.VMEM(*wide)]
            + [pltpu.SemaphoreType.DMA((4,))],
            smem=1,
            raw=grads,
            update=True,
        )
    gq, gk, gin, gv, gp, gout, gain = grads
    return (
        attended.T[None], point_grad.T[None], gin, gout.T, gq, gk, gv, gp, gain.reshape(width),
    )


def solution(mesh):
    split = P(("groups", "design"), ("geom", "head"), None)
    placed = (split, P(("groups", "design"), ("geom", "head")), split, split, split) + (P(),) * 7
    grads = (P("groups", None),) * 6 + (P("groups"),)

    return jax.shard_map(
        on_device, mesh=mesh, in_specs=placed, out_specs=(split, split) + grads, check_vma=False
    )
```

```python
import functools

import jax
import jax.numpy as jnp
from jax import lax
from jax.experimental import pallas as pl
from jax.experimental.pallas import tpu as pltpu
from jax.sharding import PartitionSpec as P


HEADS = 3
LANES = 128
DIGIT = 128
INTERPRET = False
VMEM_LIMIT = 24 << 20
BF = jnp.bfloat16
F32 = jnp.float32
GELU_C = 0.7978845608028654
GELU_A = 0.044715


def dg(a, b, ca, cb):
    return lax.dot_general(a, b, (((ca,), (cb,)), ((), ())), preferred_element_type=F32)


def split_bf(x):
    high = x.astype(BF)
    return high, (x - high.astype(F32)).astype(BF)


class Held:
    def __init__(self, value, space):
        self.value, self.space = value, space


def near(*values):
    return tuple(Held(value, pltpu.VMEM) for value in values)


def call(kernel, outs, *args, scratch=(), smem=0, final=(), raw=(), update=False, direct=()):
    held = [Held(arg, None) for arg in args[:smem]]
    held += [arg if isinstance(arg, Held) else Held(arg, pltpu.HBM) for arg in args[smem:]]
    specs = [pl.BlockSpec(memory_space=pltpu.SMEM)] * smem
    for arg in held[smem:]:
        near_spec = pl.BlockSpec(memory_space=pltpu.VMEM)
        specs.append(near_spec if arg.space is pltpu.VMEM else pl.BlockSpec())
    held += [arg if isinstance(arg, Held) else Held(arg, pltpu.HBM) for arg in raw]
    specs += [pl.BlockSpec(memory_space=pl.ANY)] * len(raw)
    operands = [
        arg.value
        if INTERPRET or arg.space is None
        else pltpu.with_memory_space_constraint(arg.value, arg.space)
        for arg in held
    ]
    if update:
        first = len(operands) - len(outs)
        aliases = {first + place: place for place in range(len(outs))} if len(raw) > 1 else {}
        return build(kernel, outs, operands, specs, scratch, range(len(outs)), aliases, pl.ANY)
    if direct:
        return build(kernel, outs, operands, specs, scratch, direct, None, pl.ANY)
    return build(kernel, outs, operands, specs, scratch, final)


def build(kernel, outs, operands, specs, scratch, final, aliases=None, space=None):
    return pl.pallas_call(
        kernel,
        out_shape=[
            jax.ShapeDtypeStruct(shape, dtype)
            if INTERPRET
            else (pltpu.HBM if place in final else pltpu.VMEM)(shape, dtype)
            for place, (shape, dtype) in enumerate(outs)
        ],
        in_specs=specs,
        out_specs=[
            pl.BlockSpec(memory_space=space if place in final else pltpu.VMEM)
            for place in range(len(outs))
        ],
        scratch_shapes=list(scratch),
        compiler_params=pltpu.CompilerParams(vmem_limit_bytes=VMEM_LIMIT),
        input_output_aliases=aliases or {},
        interpret=INTERPRET,
    )(*operands)


def round_up(n, k):
    return (n + k - 1) // k * k


def iota(shape, dim):
    return lax.broadcasted_iota(jnp.int32, shape, dim)


def gelu_terms(win, x):
    pre = dg(win, x, 0, 0)
    square = pre * pre
    tanh = jnp.tanh(pre * (GELU_C + (GELU_C * GELU_A) * square))
    return pre, square, tanh


def pool_kernel(blocks, x_ref, win_ref, wout_ref, anchor_ref, id_ref, send_ref, hsum_ref):
    width, points = x_ref.shape
    size = points // blocks
    hid = win_ref.shape[1]
    owners, rows, _ = send_ref.shape
    win = win_ref[...]
    step = 2 if blocks % 2 == 0 else 1
    hsum = jnp.zeros((hid, round_up(blocks, 8)), F32)
    for first in range(0, blocks, step):
        pre, _, tanh = gelu_terms(win, x_ref[:, pl.ds(first * size, step * size)])
        half = 0.5 * pre
        hidden = (half + half * tanh).astype(BF)
        shape = (step * size, hsum.shape[1])
        pick = (iota(shape, 1) == first + iota(shape, 0) // size).astype(F32).astype(BF)
        hsum = hsum + dg(hidden, pick, 1, 0)
    hsum = hsum.T
    hsum_ref[...] = hsum
    high, low = split_bf(hsum)
    wout = wout_ref[...]
    sums = dg(jnp.concatenate([high, low], axis=0), wout, 1, 1)
    sums = sums[: hsum.shape[0]] + sums[hsum.shape[0] :]
    ids = id_ref[...]
    digits = jnp.concatenate([ids % DIGIT, ids // DIGIT], axis=0).astype(F32)
    packed = jnp.zeros((rows, 2 * width), F32)
    packed = jnp.concatenate(
        [
            jnp.concatenate(
                [anchor_ref[...].astype(F32)]
                + ([jnp.zeros((rows - anchor_ref.shape[0], width), F32)] if rows > anchor_ref.shape[0] else []),
                axis=0,
            ),
            jnp.concatenate(
                [
                    sums[:blocks],
                    jnp.concatenate([digits, jnp.zeros((2, width - blocks), F32)], axis=1),
                    jnp.zeros((rows - blocks - 2, width), F32),
                ],
                axis=0,
            ),
        ],
        axis=1,
    ).astype(BF)
    for owner in range(owners):
        send_ref[owner] = packed


def query_kernel(
    blocks, x_ref, g_ref, wq_ref, wp_ref, wk_ref, wv_ref, gain_ref, xp_ref, win_ref,
    q_ref, dmix_ref, wk_out, wv_out, gain_out, x_out, g_out, wp_out, slope_ref,
):
    x_out[...] = x_ref[...]
    g_out[...] = g_ref[...]
    wp_out[...] = wp_ref[...]
    wk_out[...] = wk_ref[...]
    wv_out[...] = wv_ref[...]
    gain_out[...] = gain_ref[...]
    q_ref[...] = dg(wq_ref[...], x_ref[...], 0, 0).astype(BF)
    dmix_ref[...] = dg(wp_ref[...], g_ref[...], 1, 0).astype(BF)
    win = win_ref[...]
    points = xp_ref.shape[1]
    step = points // blocks * (2 if blocks % 2 == 0 else 1)
    for first in range(0, points, step):
        pre, square, tanh = gelu_terms(win, xp_ref[:, pl.ds(first, step)])
        half = 0.5 + 0.5 * tanh
        slope = half + pre * ((half * (1.0 - tanh)) * (GELU_C + (3.0 * GELU_C * GELU_A) * square))
        slope_ref[:, pl.ds(first, step)] = slope.astype(BF)


def attend_kernel(
    blocks, size, per_owner,
    got_ref, gain_ref, wk_ref, wv_ref, q_ref, dmix_ref,
    rows_ref, normed_ref, kv_ref, p_ref, ds_ref, kvt_ref,
):
    owners, rows, both = got_ref.shape
    width = both // 2
    total = owners * rows
    anchors = owners * per_owner
    got = got_ref[...].astype(F32)
    side = got[:, :, width:]
    sums = side.reshape(total, width)
    low = jnp.broadcast_to(side[:, blocks : blocks + 1, :], side.shape).reshape(total, width)
    high = jnp.broadcast_to(side[:, blocks + 1 : blocks + 2, :], side.shape).reshape(total, width)
    lane = iota((total, width), 1)
    place = iota((total, width), 0) % rows
    ids = jnp.sum(jnp.where(lane == place, low + high * DIGIT, 0.0), axis=1, keepdims=True)
    valid = (iota((total, 1), 0) % rows) < blocks
    ids = jnp.where(valid, ids, -1.0).astype(jnp.int32)
    member = (ids == iota((total, anchors), 1)).astype(F32).astype(BF)
    sums_bf = sums.astype(BF)
    pooled = dg(member, sums_bf, 0, 0)
    count = dg(member, jnp.ones((total, LANES), BF), 0, 0)[:, :1]
    inv_div = 1.0 / jnp.maximum(count * size, 1.0)
    anchor_rows = got[:, :per_owner, :width].reshape(anchors, width)
    asum = anchor_rows + pooled * inv_div
    inv = lax.rsqrt(jnp.mean(asum * asum, axis=1, keepdims=True) + 1e-6)
    gain = gain_ref[...]
    unit = asum * inv
    normed = (unit * gain).astype(BF)
    normed_ref[...] = normed
    keys = dg(normed, wk_ref[...], 1, 0).astype(BF)
    values = dg(normed, wv_ref[...], 1, 0).astype(BF)
    kv_ref[...] = jnp.concatenate([keys, values], axis=1)
    depth = width // HEADS
    scale = 1.0 / depth**0.5
    key_parts, value_parts = [], []
    for head in range(HEADS):
        part = slice(head * depth, (head + 1) * depth)
        q = q_ref[part, :]
        dmix = dmix_ref[part, :]
        scores = dg(keys[:, part], q, 1, 0) * scale
        top = jnp.max(scores, axis=0, keepdims=True)
        weight = jnp.exp(scores - top)
        probs = weight * (1.0 / jnp.sum(weight, axis=0, keepdims=True))
        probs_bf = probs.astype(BF)
        p_ref[head] = probs_bf
        dprobs = dg(values[:, part], dmix, 1, 0)
        inner = jnp.sum(probs * dprobs, axis=0, keepdims=True)
        dscore = (probs * (dprobs - inner) * scale).astype(BF)
        ds_ref[head] = dscore
        key_parts.append(dg(dscore, q, 1, 1))
        value_parts.append(dg(probs_bf, dmix, 1, 1))
    kt = jnp.concatenate(key_parts, axis=1).astype(BF)
    vt = jnp.concatenate(value_parts, axis=1).astype(BF)
    kvt_ref[...] = jnp.concatenate([kt, vt], axis=1)
    dnorm = dg(kt, wk_ref[...], 1, 1) + dg(vt, wv_ref[...], 1, 1)
    dgain = jnp.sum(dnorm * unit, axis=0, keepdims=True)
    scaled = dnorm * gain
    dsum = inv * scaled - asum * (inv * inv * inv) * jnp.mean(scaled * asum, axis=1, keepdims=True)
    dpool = (dsum * inv_div).astype(BF)
    spare = iota((total, 1), 0) % rows == blocks
    picked = jnp.where(spare, dgain, dg(member, dpool, 1, 0))
    picked = picked.reshape(owners, rows, width)
    rest = picked[:, :, LANES:]
    rest = jnp.concatenate([rest[:, : rows // 2], rest[:, rows // 2 :]], axis=2)
    rows_ref[...] = jnp.concatenate([picked[:, :, :LANES], rest], axis=1).astype(BF)


def put_rows(ref, chunk, start, value):
    done = 0
    while done < value.shape[0]:
        index, offset = divmod(start + done, chunk)
        take = min(chunk - offset, value.shape[0] - done)
        ref[index, offset : offset + take, :] = value[done : done + take]
        done += take


def get_rows(read, chunk, start, count):
    pieces = []
    done = 0
    while done < count:
        index, offset = divmod(start + done, chunk)
        take = min(chunk - offset, count - done)
        pieces.append(read(index, offset, take))
        done += take
    return pieces[0] if len(pieces) == 1 else jnp.concatenate(pieces, axis=0)


def pack_square(ref, chunk, mats):
    width = mats[0].shape[0]
    start = 0
    for first in range(0, len(mats), 2):
        left, right = mats[first : first + 2]
        pair = jnp.concatenate([left[:, LANES:], right[:, LANES:]], axis=1)
        for slot in (left[:, :LANES], right[:, :LANES], pair):
            put_rows(ref, chunk, start, slot)
            start += width


def swap_halves(head_ref, scratch, keep_ref, send_ref):
    half = keep_ref.shape[0]
    head = head_ref[0]
    keep_ref[...] = scratch[pl.ds(head * half, half)].astype(keep_ref.dtype)
    send_ref[...] = scratch[pl.ds((1 - head) * half, half)].astype(send_ref.dtype)


def fetch_kernel(mixed_ref, wp_ref, x_ref, wout_ref, win_ref, _, both_ref, win_out, out_ref, att_ref, sems):
    points = x_ref.shape[1]
    pairs = [
        (x_ref, both_ref.at[:, :points]),
        (wout_ref, both_ref.at[:, points:]),
        (win_ref, win_out),
    ]
    copies = [pltpu.make_async_copy(*pair, sems.at[place]) for place, pair in enumerate(pairs)]
    for copy in copies:
        copy.start()
    att_ref[...] = dg(wp_ref[...], mixed_ref[...], 0, 0).astype(BF)
    copies.append(pltpu.make_async_copy(att_ref, out_ref, sems.at[3]))
    copies[3].start()
    for copy in copies:
        copy.wait()


def finish_kernel(
    chunk, head_ref, p_ref, ds_ref, kv_ref, kvt_ref, normed_ref, x_ref, g_ref,
    mixed_ref, keep_ref, send_ref, dq_ref, pack_ref,
):
    width = normed_ref.shape[1]
    depth = width // HEADS
    k_ref, v_ref = kv_ref[:, :width], kv_ref[:, width:]
    kvt = dg(normed_ref[...], kvt_ref[...], 0, 0)
    for head in range(HEADS):
        part = slice(head * depth, (head + 1) * depth)
        mixed_ref[part, :] = dg(v_ref[:, part], p_ref[head], 0, 0).astype(BF)
        dq_ref[part, :] = dg(k_ref[:, part], ds_ref[head], 0, 0).astype(BF)
    mixed = mixed_ref[...]
    mats = [
        dg(x_ref[...], dq_ref[...], 1, 1),
        kvt[:, :width],
        kvt[:, width:],
        dg(mixed, g_ref[...], 1, 1),
    ]
    if pack_ref.shape[1] > chunk:
        pack_ref[:, chunk:, :] = jnp.zeros((pack_ref.shape[0], pack_ref.shape[1] - chunk, LANES), F32)
    pack_square(pack_ref, chunk, mats)
    swap_halves(head_ref, pack_ref, keep_ref, send_ref)


def back_kernel(
    blocks, chunk, head_ref, got_ref, both_ref, slope_ref, hsum_ref, *refs,
):
    dpre_ref, keep_ref, send_ref, gain_ref, pack_ref = refs[-5:]
    width = both_ref.shape[0]
    points = slope_ref.shape[1]
    size = points // blocks
    x_ref = both_ref.at[:, :points]
    wout_ref = both_ref.at[:, points:]
    total = jnp.sum(got_ref[...].astype(F32), axis=0)
    rows = total.shape[0] * 2 // 3
    rest = total[rows:]
    rest = jnp.concatenate([rest[:, : width - LANES], rest[:, width - LANES :]], axis=0)
    total = jnp.concatenate([total[:rows], rest], axis=1)
    gain_ref[...] = total[blocks : blocks + 1]
    grad = total[: hsum_ref.shape[0]].astype(BF)
    dhid = jnp.concatenate(split_bf(dg(grad, wout_ref[...], 1, 0)), axis=0)
    step = 4 if blocks % 4 == 0 else 1
    for first in range(0, blocks, step):
        cols = pl.ds(first * size, step * size)
        shape = (dhid.shape[0], step * size)
        pick = iota(shape, 0) % grad.shape[0] == first + iota(shape, 1) // size
        spread = dg(dhid, pick.astype(F32).astype(BF), 0, 0)
        dpre_ref[:, cols] = (slope_ref[:, cols].astype(F32) * spread).astype(BF)
    gin = dg(x_ref[...], dpre_ref[...], 1, 1)
    hsum = jnp.concatenate(split_bf(hsum_ref[...]), axis=0)
    gout = dg(jnp.concatenate([grad, grad], axis=0), hsum, 0, 0)
    start = 0
    for mat in (gin, gout):
        for lane in range(0, mat.shape[1], LANES):
            put_rows(pack_ref, chunk, start, mat[:, lane : lane + LANES].astype(BF))
            start += width
    swap_halves(head_ref, pack_ref, keep_ref, send_ref)


def point_grad_kernel(win_ref, dpre_ref, after_ref, out_ref):
    out_ref[...] = dg(win_ref[...], dpre_ref[...], 1, 0).astype(BF)


def design_kernel(shares, share_ref, keep_ref, got_ref, *refs):
    total_ref = refs[-1]
    total = keep_ref[...].astype(F32) + got_ref[...].astype(F32)
    total_ref[...] = total.reshape(total_ref.shape)
    for shift in range(shares):
        share = lax.rem(share_ref[0] + shift, shares)
        refs[shift][...] = total_ref[:, pl.ds(share, 1)][:, 0].astype(BF)


def join_kernel(shares, part, *refs):
    out_ref = refs[-1]
    ka_ref, kp_ref, rp_ref, gain_ref = refs[:4]
    total = ka_ref[...].astype(F32)
    for ref in refs[4:-2]:
        total = total + ref[...].astype(F32)
    groups = total.shape[0]
    top = out_ref.shape[1] - kp_ref.shape[1]
    gain = gain_ref[...] * (1.0 / groups)
    width = gain.shape[1]
    tail = [gain[:, :LANES], jnp.concatenate([gain[:, LANES:], jnp.zeros((1, 2 * LANES - width), F32)], axis=1)]
    tail = jnp.concatenate(tail + [jnp.zeros((top - part - 2, LANES), F32)], axis=0)
    for group in range(groups):
        for share in range(shares):
            piece = total[group, share * part : (share + 1) * part]
            out_ref[group * shares + share, :top, :] = jnp.concatenate([piece, tail], axis=0).astype(BF)
    out_ref[:, top:, :] = (kp_ref[...].astype(F32) + rp_ref[...].astype(F32)).astype(BF)


def sum_kernel(shares, part, top, got_ref, out_ref, gain_ref):
    peers = out_ref.shape[0]
    gain = None
    for share in range(shares):
        total = got_ref[share, :top, :].astype(F32)
        for peer in range(share + shares, peers, shares):
            total = total + got_ref[peer, :top, :].astype(F32)
        tail = total[part : part + 2]
        gain = tail if gain is None else gain + tail
        total = total[:part].astype(BF)
        for peer in range(peers):
            out_ref[peer, share * part : (share + 1) * part, :] = total
    width = gain_ref.shape[1]
    gain_ref[...] = jnp.concatenate([gain[:1], gain[1:2, : width - LANES]], axis=1)
    total = jnp.sum(got_ref[:, top:, :].astype(F32), axis=0).astype(BF)
    for peer in range(peers):
        out_ref[peer, shares * part :, :] = total


def unpack_kernel(shares, part, chunk_a, chunk_p, flip, head_ref, half_ref, gain_ref, point_ref, *refs):
    left_ref, right_ref, wide_ref, sems = refs[-4:]
    targets = refs[-12:-6]
    gain_out, point_out = refs[-6:-4]
    width = left_ref.shape[0]
    rows_a = shares * part

    def read_a(index, offset, take):
        group, share = divmod(index, shares)

        def read(source, start, count):
            row = share * part + start
            return half_ref[group * shares + source, row : row + count, :].astype(F32)

        return get_rows(read, part, offset, take)

    def read_p(index, offset, take):
        return half_ref[index, rows_a + offset : rows_a + offset + take, :].astype(F32)

    for slot in range(wide_ref.shape[1] // LANES):
        wide_ref[:, slot * LANES : (slot + 1) * LANES] = get_rows(read_p, chunk_p, slot * width, width)
    left_ref[:, :LANES] = get_rows(read_a, chunk_a, 0, width)
    right_ref[:, :LANES] = get_rows(read_a, chunk_a, width, width)
    pair = get_rows(read_a, chunk_a, 2 * width, width)
    rest = width - LANES
    left_ref[:, LANES:] = pair[:, :rest]
    right_ref[:, LANES:] = pair[:, rest:]
    if not flip:
        extras = [
            pltpu.make_async_copy(gain_ref, gain_out, sems.at[3]),
            pltpu.make_async_copy(point_ref, point_out, sems.at[4]),
        ]
        for extra in extras:
            extra.start()
    half = 1 - head_ref[0] if flip else head_ref[0]
    for which in range(2):

        @pl.when(half == which)
        def _():
            copies = [
                pltpu.make_async_copy(source, target, sems.at[place])
                for place, (source, target) in enumerate(
                    zip((left_ref, right_ref, wide_ref), targets[3 * which : 3 * which + 3])
                )
            ]
            for copy in copies:
                copy.start()
            for copy in copies:
                copy.wait()

    if not flip:
        for extra in extras:
            extra.wait()


def on_device(
    point_feats, block_anchor, anchor_feats, query_feats, out_grad, norm_gain,
    w_in, w_out, w_query, w_key, w_value, w_proj,
):
    team = ("geom", "head")
    crowd = ("geom", "design")
    owners = lax.axis_size(team)
    peers = lax.axis_size(crowd)
    xt = point_feats[0].T
    qt = query_feats[0].T
    gt = out_grad[0].T
    wot = w_out.T
    blocks = block_anchor.shape[1]
    per_owner, width = anchor_feats.shape[1:]
    points = xt.shape[1]
    queries = qt.shape[1]
    hid = w_in.shape[1]
    size = points // blocks
    anchors = owners * per_owner
    rows = round_up(max(per_owner, blocks + 2), 16)
    shares = lax.axis_size("design")
    head = lax.axis_index("head").astype(jnp.int32).reshape(1)
    share = lax.axis_index("design").astype(jnp.int32).reshape(1)
    pieces = 2 * peers
    chunk_a = 6 * width // pieces
    rows_a = round_up(chunk_a, 4 * shares)
    part = rows_a // shares
    top = round_up(part + 2, 8)
    chunk_p = 2 * width * hid // LANES // pieces

    send, hsum = call(
        functools.partial(pool_kernel, blocks),
        [((owners, rows, 2 * width), BF), ((round_up(blocks, 8), hid), F32)],
        xt, w_in, wot, anchor_feats[0], block_anchor,
    )
    got = lax.all_to_all(send, team, 0, 0, tiled=True)
    qp, dmix, wk, wv, gain_row, qn, gn, wpn, slope = call(
        functools.partial(query_kernel, blocks),
        [
            ((width, queries), BF),
            ((width, queries), BF),
            ((width, width), BF),
            ((width, width), BF),
            ((1, width), F32),
            ((width, queries), BF),
            ((width, queries), BF),
            ((width, width), BF),
            ((hid, points), BF),
        ],
        qt, gt, w_query, w_proj, w_key, w_value, norm_gain.reshape(1, width), xt, w_in,
    )
    pair_shape = (HEADS, anchors, queries)
    rows_out, normed, kv, probs, dscore, kvt = call(
        functools.partial(attend_kernel, blocks, size, per_owner),
        [
            ((owners, rows * width // LANES, LANES), BF),
            ((anchors, width), BF),
            ((anchors, 2 * width), BF),
            (pair_shape, BF),
            (pair_shape, BF),
            ((anchors, 2 * width), BF),
        ],
        *near(got, gain_row, wk, wv, qp, dmix),
    )
    back = lax.all_to_all(rows_out, team, 0, 0, tiled=True)
    shape_a = ((peers, rows_a, LANES), BF)
    mixed, keep_a, send_a = call(
        functools.partial(finish_kernel, chunk_a),
        [((width, queries), BF), shape_a, shape_a],
        head, *near(probs, dscore, kv, kvt, normed, qn, gn),
        scratch=[pltpu.VMEM((width, queries), BF), pltpu.VMEM((pieces, rows_a, LANES), F32)],
        smem=1,
    )
    both, win, attended = call(
        fetch_kernel,
        [((width, points + hid), BF), ((width, hid), BF), ((width, queries), BF)],
        *near(mixed, wpn),
        scratch=[pltpu.VMEM((width, queries), BF), pltpu.SemaphoreType.DMA((4,))],
        raw=(xt, wot, w_in) + near(send_a),
        direct=(2,),
    )
    swap = [(0, 1), (1, 0)]
    shape_p = ((peers, chunk_p, LANES), BF)
    recv_a = lax.ppermute(send_a, "head", swap)
    groups = peers // shares
    shape_d = ((groups, rows_a, LANES), BF)
    keep_d, *sends_d = call(
        functools.partial(design_kernel, shares),
        [shape_d] * shares,
        share, *near(keep_a, recv_a),
        scratch=[pltpu.VMEM((groups, shares, rows_a, LANES), F32)],
        smem=1,
    )
    recvs_d = [
        lax.ppermute(send, "design", [(i, (i + shift) % shares) for i in range(shares)])
        for shift, send in enumerate(sends_d, 1)
    ]
    dpre, keep_p, send_p, dgain = call(
        functools.partial(back_kernel, blocks, chunk_p),
        [((hid, points), BF), shape_p, shape_p, ((1, width), F32)],
        head, *near(back, both, slope, hsum),
        scratch=[pltpu.VMEM((pieces, chunk_p, LANES), BF)],
        smem=1,
        raw=near(keep_d),
    )
    recv_p = lax.ppermute(send_p, "head", swap)
    (point_grad,) = call(
        point_grad_kernel, [((width, points), BF)], *near(win, dpre), raw=near(send_p)
    )
    (joined,) = call(
        functools.partial(join_kernel, shares, part),
        [((peers, top + chunk_p, LANES), BF)],
        *near(keep_d, keep_p, recv_p, dgain, *recvs_d), raw=near(point_grad),
    )
    scattered = lax.all_to_all(joined, crowd, 0, 0, tiled=True)
    summed, gain = call(
        functools.partial(sum_kernel, shares, part, top),
        [((peers, rows_a + chunk_p, LANES), BF), ((1, width), F32)],
        *near(scattered),
    )
    mine = lax.all_to_all(summed, crowd, 0, 0, tiled=True)
    other = lax.ppermute(mine, "head", swap)
    square, wide = ((width, width), F32), ((width, hid), F32)
    grads = ()
    for flip, half in ((False, mine), (True, other)):
        grads = call(
            functools.partial(unpack_kernel, shares, part, chunk_a, chunk_p, flip),
            [square, square, wide] * 2 + [((1, width), F32), ((width, points), BF)],
            head, *near(half, gain),
            scratch=[pltpu.VMEM(*square), pltpu.VMEM(*square), pltpu.VMEM(*wide)]
            + [pltpu.SemaphoreType.DMA((5,))],
            smem=1,
            raw=near(point_grad) + tuple(grads),
            update=True,
        )
    gq, gk, gin, gv, gp, gout, gain, point_grad = grads
    return (
        attended.T[None], point_grad.T[None], gin, gout.T, gq, gk, gv, gp, gain.reshape(width),
    )


def solution(mesh):
    split = P(("groups", "design"), ("geom", "head"), None)
    placed = (split, P(("groups", "design"), ("geom", "head")), split, split, split) + (P(),) * 7
    grads = (P("groups", None),) * 6 + (P("groups"),)

    return jax.shard_map(
        on_device, mesh=mesh, in_specs=placed, out_specs=(split, split) + grads, check_vma=False
    )
```

```python
import functools

import jax
import jax.numpy as jnp
from jax import lax
from jax.experimental import pallas as pl
from jax.experimental.pallas import tpu as pltpu
from jax.sharding import PartitionSpec as P


HEADS = 3
LANES = 128
DIGIT = 128
INTERPRET = False
VMEM_LIMIT = 24 << 20
BF = jnp.bfloat16
F32 = jnp.float32
GELU_C = 0.7978845608028654
GELU_A = 0.044715
LOG2E = 1.4426950408889634


def dg(a, b, ca, cb):
    return lax.dot_general(a, b, (((ca,), (cb,)), ((), ())), preferred_element_type=F32)


def split_bf(x):
    high = x.astype(BF)
    return high, (x - high.astype(F32)).astype(BF)


class Held:
    def __init__(self, value, space):
        self.value, self.space = value, space


def near(*values):
    return tuple(Held(value, pltpu.VMEM) for value in values)


def call(kernel, outs, *args, scratch=(), smem=0, final=(), raw=(), update=False, direct=()):
    held = [Held(arg, None) for arg in args[:smem]]
    held += [arg if isinstance(arg, Held) else Held(arg, pltpu.HBM) for arg in args[smem:]]
    specs = [pl.BlockSpec(memory_space=pltpu.SMEM)] * smem
    for arg in held[smem:]:
        near_spec = pl.BlockSpec(memory_space=pltpu.VMEM)
        specs.append(near_spec if arg.space is pltpu.VMEM else pl.BlockSpec())
    held += [arg if isinstance(arg, Held) else Held(arg, pltpu.HBM) for arg in raw]
    specs += [pl.BlockSpec(memory_space=pl.ANY)] * len(raw)
    operands = [
        arg.value
        if INTERPRET or arg.space is None
        else pltpu.with_memory_space_constraint(arg.value, arg.space)
        for arg in held
    ]
    if update:
        first = len(operands) - len(outs)
        aliases = {first + place: place for place in range(len(outs))} if len(raw) > 2 else {}
        return build(kernel, outs, operands, specs, scratch, range(len(outs)), aliases, pl.ANY)
    if direct:
        return build(kernel, outs, operands, specs, scratch, direct, None, pl.ANY)
    return build(kernel, outs, operands, specs, scratch, final)


def build(kernel, outs, operands, specs, scratch, final, aliases=None, space=None):
    return pl.pallas_call(
        kernel,
        out_shape=[
            jax.ShapeDtypeStruct(shape, dtype)
            if INTERPRET
            else (pltpu.HBM if place in final else pltpu.VMEM)(shape, dtype)
            for place, (shape, dtype) in enumerate(outs)
        ],
        in_specs=specs,
        out_specs=[
            pl.BlockSpec(memory_space=space if place in final else pltpu.VMEM)
            for place in range(len(outs))
        ],
        scratch_shapes=list(scratch),
        compiler_params=pltpu.CompilerParams(vmem_limit_bytes=VMEM_LIMIT),
        input_output_aliases=aliases or {},
        interpret=INTERPRET,
    )(*operands)


def round_up(n, k):
    return (n + k - 1) // k * k


def iota(shape, dim):
    return lax.broadcasted_iota(jnp.int32, shape, dim)


def gelu_terms(win, x):
    pre = dg(win, x, 0, 0)
    square = pre * pre
    tanh = jnp.tanh(pre * (GELU_C + (GELU_C * GELU_A) * square))
    return pre, square, tanh


def pool_kernel(blocks, x_ref, win_ref, wout_ref, anchor_ref, id_ref, send_ref, hsum_ref):
    width, points = x_ref.shape
    size = points // blocks
    hid = win_ref.shape[1]
    owners, rows, _ = send_ref.shape
    win = win_ref[...]
    step = 2 if blocks % 2 == 0 else 1
    hsum = jnp.zeros((hid, round_up(blocks, 8)), F32)
    for first in range(0, blocks, step):
        pre, _, tanh = gelu_terms(win, x_ref[:, pl.ds(first * size, step * size)])
        half = 0.5 * pre
        hidden = (half + half * tanh).astype(BF)
        shape = (step * size, hsum.shape[1])
        pick = (iota(shape, 1) == first + iota(shape, 0) // size).astype(F32).astype(BF)
        hsum = hsum + dg(hidden, pick, 1, 0)
    hsum = hsum.T
    hsum_ref[...] = hsum
    high, low = split_bf(hsum)
    wout = wout_ref[...]
    sums = dg(jnp.concatenate([high, low], axis=0), wout, 1, 1)
    sums = sums[: hsum.shape[0]] + sums[hsum.shape[0] :]
    ids = id_ref[...]
    digits = jnp.concatenate([ids % DIGIT, ids // DIGIT], axis=0).astype(F32)
    packed = jnp.zeros((rows, 2 * width), F32)
    packed = jnp.concatenate(
        [
            jnp.concatenate(
                [anchor_ref[...].astype(F32)]
                + ([jnp.zeros((rows - anchor_ref.shape[0], width), F32)] if rows > anchor_ref.shape[0] else []),
                axis=0,
            ),
            jnp.concatenate(
                [
                    sums[:blocks],
                    jnp.concatenate([digits, jnp.zeros((2, width - blocks), F32)], axis=1),
                    jnp.zeros((rows - blocks - 2, width), F32),
                ],
                axis=0,
            ),
        ],
        axis=1,
    ).astype(BF)
    for owner in range(owners):
        send_ref[owner] = packed


def query_kernel(
    blocks, x_ref, g_ref, wq_ref, wp_ref, wk_ref, wv_ref, gain_ref, xp_ref, win_ref,
    q_ref, dmix_ref, wk_out, wv_out, gain_out, x_out, g_out, wp_out, slope_ref,
):
    x_out[...] = x_ref[...]
    g_out[...] = g_ref[...]
    wp_out[...] = wp_ref[...]
    wk_out[...] = wk_ref[...]
    wv_out[...] = wv_ref[...]
    gain_out[...] = gain_ref[...]
    q_ref[...] = dg(wq_ref[...], x_ref[...], 0, 0).astype(BF)
    dmix_ref[...] = dg(wp_ref[...], g_ref[...], 1, 0).astype(BF)
    win = win_ref[...]
    points = xp_ref.shape[1]
    step = points // blocks * (2 if blocks % 2 == 0 else 1)
    for first in range(0, points, step):
        pre, square, tanh = gelu_terms(win, xp_ref[:, pl.ds(first, step)])
        half = 0.5 + 0.5 * tanh
        slope = half + pre * ((half * (1.0 - tanh)) * (GELU_C + (3.0 * GELU_C * GELU_A) * square))
        slope_ref[:, pl.ds(first, step)] = slope.astype(BF)


def attend_kernel(
    blocks, size, per_owner,
    got_ref, gain_ref, wk_ref, wv_ref, q_ref, dmix_ref,
    rows_ref, normed_ref, kv_ref, p_ref, ds_ref, kvt_ref,
):
    owners, rows, both = got_ref.shape
    width = both // 2
    total = owners * rows
    anchors = owners * per_owner
    got = got_ref[...].astype(F32)
    side = got[:, :, width:]
    sums = side.reshape(total, width)
    low = jnp.broadcast_to(side[:, blocks : blocks + 1, :], side.shape).reshape(total, width)
    high = jnp.broadcast_to(side[:, blocks + 1 : blocks + 2, :], side.shape).reshape(total, width)
    lane = iota((total, width), 1)
    place = iota((total, width), 0) % rows
    ids = jnp.sum(jnp.where(lane == place, low + high * DIGIT, 0.0), axis=1, keepdims=True)
    valid = (iota((total, 1), 0) % rows) < blocks
    ids = jnp.where(valid, ids, -1.0).astype(jnp.int32)
    member = (ids == iota((total, anchors), 1)).astype(F32).astype(BF)
    sums_bf = sums.astype(BF)
    pooled = dg(member, sums_bf, 0, 0)
    count = dg(member, jnp.ones((total, LANES), BF), 0, 0)[:, :1]
    inv_div = 1.0 / jnp.maximum(count * size, 1.0)
    anchor_rows = got[:, :per_owner, :width].reshape(anchors, width)
    asum = anchor_rows + pooled * inv_div
    inv = lax.rsqrt(jnp.mean(asum * asum, axis=1, keepdims=True) + 1e-6)
    gain = gain_ref[...]
    unit = asum * inv
    normed = (unit * gain).astype(BF)
    normed_ref[...] = normed
    keys = dg(normed, wk_ref[...], 1, 0).astype(BF)
    values = dg(normed, wv_ref[...], 1, 0).astype(BF)
    kv_ref[...] = jnp.concatenate([keys, values], axis=1)
    depth = width // HEADS
    scale = 1.0 / depth**0.5
    key_parts, value_parts = [], []
    for head in range(HEADS):
        part = slice(head * depth, (head + 1) * depth)
        q = q_ref[part, :]
        dmix = dmix_ref[part, :]
        scores = dg(keys[:, part], q, 1, 0)
        top = jnp.max(scores, axis=0, keepdims=True)
        weight = jnp.exp2((scores - top) * (scale * LOG2E))
        probs = weight * (1.0 / jnp.sum(weight, axis=0, keepdims=True))
        probs_bf = probs.astype(BF)
        p_ref[head] = probs_bf
        dprobs = dg(values[:, part], dmix, 1, 0)
        inner = jnp.sum(probs * dprobs, axis=0, keepdims=True)
        dscore = (probs * (dprobs - inner) * scale).astype(BF)
        ds_ref[head] = dscore
        key_parts.append(dg(dscore, q, 1, 1))
        value_parts.append(dg(probs_bf, dmix, 1, 1))
    kt = jnp.concatenate(key_parts, axis=1).astype(BF)
    vt = jnp.concatenate(value_parts, axis=1).astype(BF)
    kvt_ref[...] = jnp.concatenate([kt, vt], axis=1)
    dnorm = dg(kt, wk_ref[...], 1, 1) + dg(vt, wv_ref[...], 1, 1)
    dgain = jnp.sum(dnorm * unit, axis=0, keepdims=True)
    scaled = dnorm * gain
    dsum = inv * scaled - asum * (inv * inv * inv) * jnp.mean(scaled * asum, axis=1, keepdims=True)
    dpool = (dsum * inv_div).astype(BF)
    spare = iota((total, 1), 0) % rows == blocks
    picked = jnp.where(spare, dgain, dg(member, dpool, 1, 0))
    picked = picked.reshape(owners, rows, width)
    rest = picked[:, :, LANES:]
    rest = jnp.concatenate([rest[:, : rows // 2], rest[:, rows // 2 :]], axis=2)
    rows_ref[...] = jnp.concatenate([picked[:, :, :LANES], rest], axis=1).astype(BF)


def put_rows(ref, chunk, start, value):
    done = 0
    while done < value.shape[0]:
        index, offset = divmod(start + done, chunk)
        take = min(chunk - offset, value.shape[0] - done)
        ref[index, offset : offset + take, :] = value[done : done + take]
        done += take


def get_rows(read, chunk, start, count):
    pieces = []
    done = 0
    while done < count:
        index, offset = divmod(start + done, chunk)
        take = min(chunk - offset, count - done)
        pieces.append(read(index, offset, take))
        done += take
    return pieces[0] if len(pieces) == 1 else jnp.concatenate(pieces, axis=0)


def pack_square(ref, chunk, mats):
    width = mats[0].shape[0]
    start = 0
    for first in range(0, len(mats), 2):
        left, right = mats[first : first + 2]
        pair = jnp.concatenate([left[:, LANES:], right[:, LANES:]], axis=1)
        for slot in (left[:, :LANES], right[:, :LANES], pair):
            put_rows(ref, chunk, start, slot)
            start += width


def swap_halves(head_ref, scratch, keep_ref, send_ref):
    half = keep_ref.shape[0]
    head = head_ref[0]
    keep_ref[...] = scratch[pl.ds(head * half, half)].astype(keep_ref.dtype)
    send_ref[...] = scratch[pl.ds((1 - head) * half, half)].astype(send_ref.dtype)


def fetch_kernel(mixed_ref, wp_ref, x_ref, wout_ref, win_ref, _, both_ref, win_out, att_ref, sems):
    points = x_ref.shape[1]
    pairs = [
        (x_ref, both_ref.at[:, :points]),
        (wout_ref, both_ref.at[:, points:]),
        (win_ref, win_out),
    ]
    copies = [pltpu.make_async_copy(*pair, sems.at[place]) for place, pair in enumerate(pairs)]
    for copy in copies:
        copy.start()
    att_ref[...] = dg(wp_ref[...], mixed_ref[...], 0, 0).astype(BF)
    for copy in copies:
        copy.wait()


def finish_kernel(
    chunk, head_ref, p_ref, ds_ref, kv_ref, kvt_ref, normed_ref, x_ref, g_ref,
    mixed_ref, keep_ref, send_ref, dq_ref, pack_ref,
):
    width = normed_ref.shape[1]
    depth = width // HEADS
    k_ref, v_ref = kv_ref[:, :width], kv_ref[:, width:]
    kvt = dg(normed_ref[...], kvt_ref[...], 0, 0)
    for head in range(HEADS):
        part = slice(head * depth, (head + 1) * depth)
        mixed_ref[part, :] = dg(v_ref[:, part], p_ref[head], 0, 0).astype(BF)
        dq_ref[part, :] = dg(k_ref[:, part], ds_ref[head], 0, 0).astype(BF)
    mixed = mixed_ref[...]
    mats = [
        dg(x_ref[...], dq_ref[...], 1, 1),
        kvt[:, :width],
        kvt[:, width:],
        dg(mixed, g_ref[...], 1, 1),
    ]
    if pack_ref.shape[1] > chunk:
        pack_ref[:, chunk:, :] = jnp.zeros((pack_ref.shape[0], pack_ref.shape[1] - chunk, LANES), F32)
    pack_square(pack_ref, chunk, mats)
    swap_halves(head_ref, pack_ref, keep_ref, send_ref)


def back_kernel(
    blocks, chunk, head_ref, got_ref, both_ref, slope_ref, hsum_ref, *refs,
):
    dpre_ref, keep_ref, send_ref, gain_ref, pack_ref = refs[-5:]
    width = both_ref.shape[0]
    points = slope_ref.shape[1]
    size = points // blocks
    x_ref = both_ref.at[:, :points]
    wout_ref = both_ref.at[:, points:]
    total = jnp.sum(got_ref[...].astype(F32), axis=0)
    rows = total.shape[0] * 2 // 3
    rest = total[rows:]
    rest = jnp.concatenate([rest[:, : width - LANES], rest[:, width - LANES :]], axis=0)
    total = jnp.concatenate([total[:rows], rest], axis=1)
    gain_ref[...] = total[blocks : blocks + 1]
    grad = total[: hsum_ref.shape[0]].astype(BF)
    dhid = jnp.concatenate(split_bf(dg(grad, wout_ref[...], 1, 0)), axis=0)
    step = 4 if blocks % 4 == 0 else 1
    for first in range(0, blocks, step):
        cols = pl.ds(first * size, step * size)
        shape = (dhid.shape[0], step * size)
        pick = iota(shape, 0) % grad.shape[0] == first + iota(shape, 1) // size
        spread = dg(dhid, pick.astype(F32).astype(BF), 0, 0)
        dpre_ref[:, cols] = (slope_ref[:, cols].astype(F32) * spread).astype(BF)
    gin = dg(x_ref[...], dpre_ref[...], 1, 1)
    hsum = jnp.concatenate(split_bf(hsum_ref[...]), axis=0)
    gout = dg(jnp.concatenate([grad, grad], axis=0), hsum, 0, 0)
    start = 0
    for mat in (gin, gout):
        for lane in range(0, mat.shape[1], LANES):
            put_rows(pack_ref, chunk, start, mat[:, lane : lane + LANES].astype(BF))
            start += width
    swap_halves(head_ref, pack_ref, keep_ref, send_ref)


def point_grad_kernel(win_ref, dpre_ref, after_ref, out_ref):
    out_ref[...] = dg(win_ref[...], dpre_ref[...], 1, 0).astype(BF)


def design_kernel(shares, share_ref, keep_ref, got_ref, *refs):
    total_ref = refs[-1]
    total = keep_ref[...].astype(F32) + got_ref[...].astype(F32)
    total_ref[...] = total.reshape(total_ref.shape)
    for shift in range(shares):
        share = lax.rem(share_ref[0] + shift, shares)
        refs[shift][...] = total_ref[:, pl.ds(share, 1)][:, 0].astype(BF)


def join_kernel(shares, part, *refs):
    out_ref = refs[-1]
    ka_ref, kp_ref, rp_ref, gain_ref = refs[:4]
    total = ka_ref[...].astype(F32)
    for ref in refs[4:-2]:
        total = total + ref[...].astype(F32)
    groups = total.shape[0]
    top = out_ref.shape[1] - kp_ref.shape[1]
    gain = gain_ref[...] * (1.0 / groups)
    width = gain.shape[1]
    tail = [gain[:, :LANES], jnp.concatenate([gain[:, LANES:], jnp.zeros((1, 2 * LANES - width), F32)], axis=1)]
    tail = jnp.concatenate(tail + [jnp.zeros((top - part - 2, LANES), F32)], axis=0)
    for group in range(groups):
        for share in range(shares):
            piece = total[group, share * part : (share + 1) * part]
            out_ref[group * shares + share, :top, :] = jnp.concatenate([piece, tail], axis=0).astype(BF)
    out_ref[:, top:, :] = (kp_ref[...].astype(F32) + rp_ref[...].astype(F32)).astype(BF)


def sum_kernel(shares, part, top, got_ref, out_ref, gain_ref):
    peers = out_ref.shape[0]
    gain = None
    for share in range(shares):
        total = got_ref[share, :top, :].astype(F32)
        for peer in range(share + shares, peers, shares):
            total = total + got_ref[peer, :top, :].astype(F32)
        tail = total[part : part + 2]
        gain = tail if gain is None else gain + tail
        total = total[:part].astype(BF)
        for peer in range(peers):
            out_ref[peer, share * part : (share + 1) * part, :] = total
    width = gain_ref.shape[1]
    gain_ref[...] = jnp.concatenate([gain[:1], gain[1:2, : width - LANES]], axis=1)
    total = jnp.sum(got_ref[:, top:, :].astype(F32), axis=0).astype(BF)
    for peer in range(peers):
        out_ref[peer, shares * part :, :] = total


def unpack_kernel(shares, part, chunk_a, chunk_p, flip, head_ref, half_ref, gain_ref, att_ref, point_ref, *refs):
    left_ref, right_ref, wide_ref, sems = refs[-4:]
    targets = refs[-13:-7]
    gain_out, point_out, att_out = refs[-7:-4]
    width = left_ref.shape[0]
    rows_a = shares * part

    def read_a(index, offset, take):
        group, share = divmod(index, shares)

        def read(source, start, count):
            row = share * part + start
            return half_ref[group * shares + source, row : row + count, :].astype(F32)

        return get_rows(read, part, offset, take)

    def read_p(index, offset, take):
        return half_ref[index, rows_a + offset : rows_a + offset + take, :].astype(F32)

    for slot in range(wide_ref.shape[1] // LANES):
        wide_ref[:, slot * LANES : (slot + 1) * LANES] = get_rows(read_p, chunk_p, slot * width, width)
    left_ref[:, :LANES] = get_rows(read_a, chunk_a, 0, width)
    right_ref[:, :LANES] = get_rows(read_a, chunk_a, width, width)
    pair = get_rows(read_a, chunk_a, 2 * width, width)
    rest = width - LANES
    left_ref[:, LANES:] = pair[:, :rest]
    right_ref[:, LANES:] = pair[:, rest:]
    if not flip:
        extras = [
            pltpu.make_async_copy(gain_ref, gain_out, sems.at[3]),
            pltpu.make_async_copy(point_ref, point_out, sems.at[4]),
            pltpu.make_async_copy(att_ref, att_out, sems.at[5]),
        ]
        for extra in extras:
            extra.start()
    half = 1 - head_ref[0] if flip else head_ref[0]
    for which in range(2):

        @pl.when(half == which)
        def _():
            copies = [
                pltpu.make_async_copy(source, target, sems.at[place])
                for place, (source, target) in enumerate(
                    zip((left_ref, right_ref, wide_ref), targets[3 * which : 3 * which + 3])
                )
            ]
            for copy in copies:
                copy.start()
            for copy in copies:
                copy.wait()

    if not flip:
        for extra in extras:
            extra.wait()


def on_device(
    point_feats, block_anchor, anchor_feats, query_feats, out_grad, norm_gain,
    w_in, w_out, w_query, w_key, w_value, w_proj,
):
    team = ("geom", "head")
    crowd = ("geom", "design")
    owners = lax.axis_size(team)
    peers = lax.axis_size(crowd)
    xt = point_feats[0].T
    qt = query_feats[0].T
    gt = out_grad[0].T
    wot = w_out.T
    blocks = block_anchor.shape[1]
    per_owner, width = anchor_feats.shape[1:]
    points = xt.shape[1]
    queries = qt.shape[1]
    hid = w_in.shape[1]
    size = points // blocks
    anchors = owners * per_owner
    rows = round_up(max(per_owner, blocks + 2), 16)
    shares = lax.axis_size("design")
    head = lax.axis_index("head").astype(jnp.int32).reshape(1)
    share = lax.axis_index("design").astype(jnp.int32).reshape(1)
    pieces = 2 * peers
    chunk_a = 6 * width // pieces
    rows_a = round_up(chunk_a, 4 * shares)
    part = rows_a // shares
    top = round_up(part + 2, 8)
    chunk_p = 2 * width * hid // LANES // pieces

    send, hsum = call(
        functools.partial(pool_kernel, blocks),
        [((owners, rows, 2 * width), BF), ((round_up(blocks, 8), hid), F32)],
        xt, w_in, wot, anchor_feats[0], block_anchor,
    )
    got = lax.all_to_all(send, team, 0, 0, tiled=True)
    qp, dmix, wk, wv, gain_row, qn, gn, wpn, slope = call(
        functools.partial(query_kernel, blocks),
        [
            ((width, queries), BF),
            ((width, queries), BF),
            ((width, width), BF),
            ((width, width), BF),
            ((1, width), F32),
            ((width, queries), BF),
            ((width, queries), BF),
            ((width, width), BF),
            ((hid, points), BF),
        ],
        qt, gt, w_query, w_proj, w_key, w_value, norm_gain.reshape(1, width), xt, w_in,
    )
    pair_shape = (HEADS, anchors, queries)
    rows_out, normed, kv, probs, dscore, kvt = call(
        functools.partial(attend_kernel, blocks, size, per_owner),
        [
            ((owners, rows * width // LANES, LANES), BF),
            ((anchors, width), BF),
            ((anchors, 2 * width), BF),
            (pair_shape, BF),
            (pair_shape, BF),
            ((anchors, 2 * width), BF),
        ],
        *near(got, gain_row, wk, wv, qp, dmix),
    )
    back = lax.all_to_all(rows_out, team, 0, 0, tiled=True)
    shape_a = ((peers, rows_a, LANES), BF)
    mixed, keep_a, send_a = call(
        functools.partial(finish_kernel, chunk_a),
        [((width, queries), BF), shape_a, shape_a],
        head, *near(probs, dscore, kv, kvt, normed, qn, gn),
        scratch=[pltpu.VMEM((width, queries), BF), pltpu.VMEM((pieces, rows_a, LANES), F32)],
        smem=1,
    )
    both, win, attended = call(
        fetch_kernel,
        [((width, points + hid), BF), ((width, hid), BF), ((width, queries), BF)],
        *near(mixed, wpn),
        scratch=[pltpu.SemaphoreType.DMA((3,))],
        raw=(xt, wot, w_in) + near(send_a),
    )
    swap = [(0, 1), (1, 0)]
    shape_p = ((peers, chunk_p, LANES), BF)
    recv_a = lax.ppermute(send_a, "head", swap)
    groups = peers // shares
    shape_d = ((groups, rows_a, LANES), BF)
    keep_d, *sends_d = call(
        functools.partial(design_kernel, shares),
        [shape_d] * shares,
        share, *near(keep_a, recv_a),
        scratch=[pltpu.VMEM((groups, shares, rows_a, LANES), F32)],
        smem=1,
    )
    recvs_d = [
        lax.ppermute(send, "design", [(i, (i + shift) % shares) for i in range(shares)])
        for shift, send in enumerate(sends_d, 1)
    ]
    dpre, keep_p, send_p, dgain = call(
        functools.partial(back_kernel, blocks, chunk_p),
        [((hid, points), BF), shape_p, shape_p, ((1, width), F32)],
        head, *near(back, both, slope, hsum),
        scratch=[pltpu.VMEM((pieces, chunk_p, LANES), BF)],
        smem=1,
        raw=near(keep_d),
    )
    recv_p = lax.ppermute(send_p, "head", swap)
    (point_grad,) = call(
        point_grad_kernel, [((width, points), BF)], *near(win, dpre), raw=near(send_p)
    )
    (joined,) = call(
        functools.partial(join_kernel, shares, part),
        [((peers, top + chunk_p, LANES), BF)],
        *near(keep_d, keep_p, recv_p, dgain, *recvs_d), raw=near(point_grad),
    )
    scattered = lax.all_to_all(joined, crowd, 0, 0, tiled=True)
    summed, gain = call(
        functools.partial(sum_kernel, shares, part, top),
        [((peers, rows_a + chunk_p, LANES), BF), ((1, width), F32)],
        *near(scattered),
    )
    mine = lax.all_to_all(summed, crowd, 0, 0, tiled=True)
    other = lax.ppermute(mine, "head", swap)
    square, wide = ((width, width), F32), ((width, hid), F32)
    grads = ()
    for flip, half in ((False, mine), (True, other)):
        grads = call(
            functools.partial(unpack_kernel, shares, part, chunk_a, chunk_p, flip),
            [square, square, wide] * 2 + [((1, width), F32), ((width, points), BF), ((width, queries), BF)],
            head, *near(half, gain),
            scratch=[pltpu.VMEM(*square), pltpu.VMEM(*square), pltpu.VMEM(*wide)]
            + [pltpu.SemaphoreType.DMA((6,))],
            smem=1,
            raw=near(attended, point_grad) + tuple(grads),
            update=True,
        )
    gq, gk, gin, gv, gp, gout, gain, point_grad, attended = grads
    return (
        attended.T[None], point_grad.T[None], gin, gout.T, gq, gk, gv, gp, gain.reshape(width),
    )


def solution(mesh):
    split = P(("groups", "design"), ("geom", "head"), None)
    placed = (split, P(("groups", "design"), ("geom", "head")), split, split, split) + (P(),) * 7
    grads = (P("groups", None),) * 6 + (P("groups"),)

    return jax.shard_map(
        on_device, mesh=mesh, in_specs=placed, out_specs=(split, split) + grads, check_vma=False
    )
```

```python
import functools

import jax
import jax.numpy as jnp
from jax import lax
from jax.experimental import pallas as pl
from jax.experimental.pallas import tpu as pltpu
from jax.sharding import PartitionSpec as P


HEADS = 3
LANES = 128
DIGIT = 128
INTERPRET = False
VMEM_LIMIT = 24 << 20
BF = jnp.bfloat16
F32 = jnp.float32
GELU_C = 0.7978845608028654
GELU_A = 0.044715
LOG2E = 1.4426950408889634


def dg(a, b, ca, cb):
    return lax.dot_general(a, b, (((ca,), (cb,)), ((), ())), preferred_element_type=F32)


def split_bf(x):
    high = x.astype(BF)
    return high, (x - high.astype(F32)).astype(BF)


class Held:
    def __init__(self, value, space):
        self.value, self.space = value, space


def near(*values):
    return tuple(Held(value, pltpu.VMEM) for value in values)


def call(kernel, outs, *args, scratch=(), smem=0, final=(), raw=(), update=False, direct=()):
    held = [Held(arg, None) for arg in args[:smem]]
    held += [arg if isinstance(arg, Held) else Held(arg, pltpu.HBM) for arg in args[smem:]]
    specs = [pl.BlockSpec(memory_space=pltpu.SMEM)] * smem
    for arg in held[smem:]:
        near_spec = pl.BlockSpec(memory_space=pltpu.VMEM)
        specs.append(near_spec if arg.space is pltpu.VMEM else pl.BlockSpec())
    held += [arg if isinstance(arg, Held) else Held(arg, pltpu.HBM) for arg in raw]
    specs += [pl.BlockSpec(memory_space=pl.ANY)] * len(raw)
    operands = [
        arg.value
        if INTERPRET or arg.space is None
        else pltpu.with_memory_space_constraint(arg.value, arg.space)
        for arg in held
    ]
    if update:
        first = len(operands) - len(outs)
        aliases = {first + place: place for place in range(len(outs))} if len(raw) > 2 else {}
        return build(kernel, outs, operands, specs, scratch, range(len(outs)), aliases, pl.ANY)
    if direct:
        return build(kernel, outs, operands, specs, scratch, direct, None, pl.ANY)
    return build(kernel, outs, operands, specs, scratch, final)


def build(kernel, outs, operands, specs, scratch, final, aliases=None, space=None):
    return pl.pallas_call(
        kernel,
        out_shape=[
            jax.ShapeDtypeStruct(shape, dtype)
            if INTERPRET
            else (pltpu.HBM if place in final else pltpu.VMEM)(shape, dtype)
            for place, (shape, dtype) in enumerate(outs)
        ],
        in_specs=specs,
        out_specs=[
            pl.BlockSpec(memory_space=space if place in final else pltpu.VMEM)
            for place in range(len(outs))
        ],
        scratch_shapes=list(scratch),
        compiler_params=pltpu.CompilerParams(vmem_limit_bytes=VMEM_LIMIT),
        input_output_aliases=aliases or {},
        interpret=INTERPRET,
    )(*operands)


def round_up(n, k):
    return (n + k - 1) // k * k


def iota(shape, dim):
    return lax.broadcasted_iota(jnp.int32, shape, dim)


def gelu_terms(win, x):
    pre = dg(win, x, 0, 0)
    square = pre * pre
    tanh = jnp.tanh(pre * (GELU_C + (GELU_C * GELU_A) * square))
    return pre, square, tanh


def pool_kernel(blocks, x_ref, win_ref, wout_ref, anchor_ref, id_ref, send_ref, hsum_ref):
    width, points = x_ref.shape
    size = points // blocks
    hid = win_ref.shape[1]
    owners, rows, _ = send_ref.shape
    win = win_ref[...]
    step = 2 if blocks % 2 == 0 else 1
    hsum = jnp.zeros((hid, round_up(blocks, 8)), F32)
    for first in range(0, blocks, step):
        pre, _, tanh = gelu_terms(win, x_ref[:, pl.ds(first * size, step * size)])
        half = 0.5 * pre
        hidden = (half + half * tanh).astype(BF)
        shape = (step * size, hsum.shape[1])
        pick = (iota(shape, 1) == first + iota(shape, 0) // size).astype(F32).astype(BF)
        hsum = hsum + dg(hidden, pick, 1, 0)
    hsum = hsum.T
    hsum_ref[...] = hsum
    high, low = split_bf(hsum)
    wout = wout_ref[...]
    sums = dg(jnp.concatenate([high, low], axis=0), wout, 1, 1)
    sums = sums[: hsum.shape[0]] + sums[hsum.shape[0] :]
    ids = id_ref[...]
    digits = jnp.concatenate([ids % DIGIT, ids // DIGIT], axis=0).astype(F32)
    packed = jnp.zeros((rows, 2 * width), F32)
    packed = jnp.concatenate(
        [
            jnp.concatenate(
                [anchor_ref[...].astype(F32)]
                + ([jnp.zeros((rows - anchor_ref.shape[0], width), F32)] if rows > anchor_ref.shape[0] else []),
                axis=0,
            ),
            jnp.concatenate(
                [
                    sums[:blocks],
                    jnp.concatenate([digits, jnp.zeros((2, width - blocks), F32)], axis=1),
                    jnp.zeros((rows - blocks - 2, width), F32),
                ],
                axis=0,
            ),
        ],
        axis=1,
    ).astype(BF)
    for owner in range(owners):
        send_ref[owner] = packed


def query_kernel(
    blocks, x_ref, g_ref, wq_ref, wp_ref, wk_ref, wv_ref, gain_ref, xp_ref, win_ref,
    q_ref, dmix_ref, wk_out, wv_out, gain_out, x_out, g_out, wp_out, slope_ref,
):
    x_out[...] = x_ref[...]
    g_out[...] = g_ref[...]
    wp_out[...] = wp_ref[...]
    wk_out[...] = wk_ref[...]
    wv_out[...] = wv_ref[...]
    gain_out[...] = gain_ref[...]
    q_ref[...] = dg(wq_ref[...], x_ref[...], 0, 0).astype(BF)
    dmix_ref[...] = dg(wp_ref[...], g_ref[...], 1, 0).astype(BF)
    win = win_ref[...]
    points = xp_ref.shape[1]
    step = points // blocks * (2 if blocks % 2 == 0 else 1)
    for first in range(0, points, step):
        pre, square, tanh = gelu_terms(win, xp_ref[:, pl.ds(first, step)])
        half = 0.5 + 0.5 * tanh
        slope = half + pre * ((half * (1.0 - tanh)) * (GELU_C + (3.0 * GELU_C * GELU_A) * square))
        slope_ref[:, pl.ds(first, step)] = slope.astype(BF)


def attend_kernel(
    blocks, size, per_owner,
    got_ref, gain_ref, wk_ref, wv_ref, q_ref, dmix_ref,
    rows_ref, normed_ref, kv_ref, p_ref, ds_ref, kvt_ref,
):
    owners, rows, both = got_ref.shape
    width = both // 2
    total = owners * rows
    anchors = owners * per_owner
    got = got_ref[...].astype(F32)
    side = got[:, :, width:]
    sums = side.reshape(total, width)
    low = jnp.broadcast_to(side[:, blocks : blocks + 1, :], side.shape).reshape(total, width)
    high = jnp.broadcast_to(side[:, blocks + 1 : blocks + 2, :], side.shape).reshape(total, width)
    lane = iota((total, width), 1)
    place = iota((total, width), 0) % rows
    ids = jnp.sum(jnp.where(lane == place, low + high * DIGIT, 0.0), axis=1, keepdims=True)
    valid = (iota((total, 1), 0) % rows) < blocks
    ids = jnp.where(valid, ids, -1.0).astype(jnp.int32)
    member = (ids == iota((total, anchors), 1)).astype(F32).astype(BF)
    sums_bf = sums.astype(BF)
    pooled = dg(member, sums_bf, 0, 0)
    count = dg(member, jnp.ones((total, LANES), BF), 0, 0)[:, :1]
    inv_div = 1.0 / jnp.maximum(count * size, 1.0)
    anchor_rows = got[:, :per_owner, :width].reshape(anchors, width)
    asum = anchor_rows + pooled * inv_div
    inv = lax.rsqrt(jnp.mean(asum * asum, axis=1, keepdims=True) + 1e-6)
    gain = gain_ref[...]
    unit = asum * inv
    normed = (unit * gain).astype(BF)
    normed_ref[...] = normed
    keys = dg(normed, wk_ref[...], 1, 0).astype(BF)
    values = dg(normed, wv_ref[...], 1, 0).astype(BF)
    kv_ref[...] = jnp.concatenate([keys, values], axis=1)
    depth = width // HEADS
    scale = 1.0 / depth**0.5
    key_parts, value_parts = [], []
    for head in range(HEADS):
        part = slice(head * depth, (head + 1) * depth)
        q = q_ref[part, :]
        dmix = dmix_ref[part, :]
        scores = dg(keys[:, part], q, 1, 0)
        top = jnp.max(scores, axis=0, keepdims=True)
        weight = jnp.exp2((scores - top) * (scale * LOG2E))
        probs = weight * (1.0 / jnp.sum(weight, axis=0, keepdims=True))
        probs_bf = probs.astype(BF)
        p_ref[head] = probs_bf
        dprobs = dg(values[:, part], dmix, 1, 0)
        inner = jnp.sum(probs * dprobs, axis=0, keepdims=True)
        dscore = (probs * (dprobs - inner) * scale).astype(BF)
        ds_ref[head] = dscore
        key_parts.append(dg(dscore, q, 1, 1))
        value_parts.append(dg(probs_bf, dmix, 1, 1))
    kt = jnp.concatenate(key_parts, axis=1).astype(BF)
    vt = jnp.concatenate(value_parts, axis=1).astype(BF)
    kvt_ref[...] = jnp.concatenate([kt, vt], axis=1)
    dnorm = dg(kt, wk_ref[...], 1, 1) + dg(vt, wv_ref[...], 1, 1)
    dgain = jnp.sum(dnorm * unit, axis=0, keepdims=True)
    scaled = dnorm * gain
    dsum = inv * scaled - asum * (inv * inv * inv) * jnp.mean(scaled * asum, axis=1, keepdims=True)
    dpool = (dsum * inv_div).astype(BF)
    spare = iota((total, 1), 0) % rows == blocks
    picked = jnp.where(spare, dgain, dg(member, dpool, 1, 0))
    picked = picked.reshape(owners, rows, width)
    rest = picked[:, :, LANES:]
    rest = jnp.concatenate([rest[:, : rows // 2], rest[:, rows // 2 :]], axis=2)
    rows_ref[...] = jnp.concatenate([picked[:, :, :LANES], rest], axis=1).astype(BF)


def put_rows(ref, chunk, start, value):
    done = 0
    while done < value.shape[0]:
        index, offset = divmod(start + done, chunk)
        take = min(chunk - offset, value.shape[0] - done)
        ref[index, offset : offset + take, :] = value[done : done + take]
        done += take


def get_rows(read, chunk, start, count):
    pieces = []
    done = 0
    while done < count:
        index, offset = divmod(start + done, chunk)
        take = min(chunk - offset, count - done)
        pieces.append(read(index, offset, take))
        done += take
    return pieces[0] if len(pieces) == 1 else jnp.concatenate(pieces, axis=0)


def pack_square(ref, chunk, mats):
    width = mats[0].shape[0]
    start = 0
    for first in range(0, len(mats), 2):
        left, right = mats[first : first + 2]
        pair = jnp.concatenate([left[:, LANES:], right[:, LANES:]], axis=1)
        for slot in (left[:, :LANES], right[:, :LANES], pair):
            put_rows(ref, chunk, start, slot.astype(BF))
            start += width


def swap_halves(head_ref, scratch, keep_ref, send_ref):
    half = keep_ref.shape[0]
    head = head_ref[0]
    keep_ref[...] = scratch[pl.ds(head * half, half)].astype(keep_ref.dtype)
    send_ref[...] = scratch[pl.ds((1 - head) * half, half)].astype(send_ref.dtype)


def fetch_kernel(mixed_ref, wp_ref, x_ref, wout_ref, win_ref, _, both_ref, win_out, att_ref, sems):
    points = x_ref.shape[1]
    pairs = [
        (x_ref, both_ref.at[:, :points]),
        (wout_ref, both_ref.at[:, points:]),
        (win_ref, win_out),
    ]
    copies = [pltpu.make_async_copy(*pair, sems.at[place]) for place, pair in enumerate(pairs)]
    for copy in copies:
        copy.start()
    att_ref[...] = dg(wp_ref[...], mixed_ref[...], 0, 0).astype(BF)
    for copy in copies:
        copy.wait()


def finish_kernel(
    chunk, head_ref, p_ref, ds_ref, kv_ref, kvt_ref, normed_ref, x_ref, g_ref,
    mixed_ref, keep_ref, send_ref, dq_ref, pack_ref,
):
    width = normed_ref.shape[1]
    depth = width // HEADS
    k_ref, v_ref = kv_ref[:, :width], kv_ref[:, width:]
    kvt = dg(normed_ref[...], kvt_ref[...], 0, 0)
    for head in range(HEADS):
        part = slice(head * depth, (head + 1) * depth)
        mixed_ref[part, :] = dg(v_ref[:, part], p_ref[head], 0, 0).astype(BF)
        dq_ref[part, :] = dg(k_ref[:, part], ds_ref[head], 0, 0).astype(BF)
    mixed = mixed_ref[...]
    mats = [
        dg(x_ref[...], dq_ref[...], 1, 1),
        kvt[:, :width],
        kvt[:, width:],
        dg(mixed, g_ref[...], 1, 1),
    ]
    if pack_ref.shape[1] > chunk:
        pack_ref[:, chunk:, :] = jnp.zeros((pack_ref.shape[0], pack_ref.shape[1] - chunk, LANES), BF)
    pack_square(pack_ref, chunk, mats)
    swap_halves(head_ref, pack_ref, keep_ref, send_ref)


def back_kernel(
    blocks, chunk, head_ref, got_ref, both_ref, slope_ref, hsum_ref, *refs,
):
    dpre_ref, keep_ref, send_ref, gain_ref, pack_ref = refs[-5:]
    width = both_ref.shape[0]
    points = slope_ref.shape[1]
    size = points // blocks
    x_ref = both_ref.at[:, :points]
    wout_ref = both_ref.at[:, points:]
    total = jnp.sum(got_ref[...].astype(F32), axis=0)
    rows = total.shape[0] * 2 // 3
    rest = total[rows:]
    rest = jnp.concatenate([rest[:, : width - LANES], rest[:, width - LANES :]], axis=0)
    total = jnp.concatenate([total[:rows], rest], axis=1)
    gain_ref[...] = total[blocks : blocks + 1]
    grad = total[: hsum_ref.shape[0]].astype(BF)
    dhid = jnp.concatenate(split_bf(dg(grad, wout_ref[...], 1, 0)), axis=0)
    step = 4 if blocks % 4 == 0 else 1
    for first in range(0, blocks, step):
        cols = pl.ds(first * size, step * size)
        shape = (dhid.shape[0], step * size)
        pick = iota(shape, 0) % grad.shape[0] == first + iota(shape, 1) // size
        spread = dg(dhid, pick.astype(F32).astype(BF), 0, 0)
        dpre_ref[:, cols] = (slope_ref[:, cols].astype(F32) * spread).astype(BF)
    gin = dg(x_ref[...], dpre_ref[...], 1, 1)
    hsum = jnp.concatenate(split_bf(hsum_ref[...]), axis=0)
    gout = dg(jnp.concatenate([grad, grad], axis=0), hsum, 0, 0)
    start = 0
    for mat in (gin, gout):
        for lane in range(0, mat.shape[1], LANES):
            put_rows(pack_ref, chunk, start, mat[:, lane : lane + LANES].astype(BF))
            start += width
    swap_halves(head_ref, pack_ref, keep_ref, send_ref)


def point_grad_kernel(win_ref, dpre_ref, after_ref, out_ref):
    out_ref[...] = dg(win_ref[...], dpre_ref[...], 1, 0).astype(BF)


def design_kernel(shares, share_ref, keep_ref, got_ref, *refs):
    total_ref = refs[-1]
    total = keep_ref[...].astype(F32) + got_ref[...].astype(F32)
    total_ref[...] = total.reshape(total_ref.shape)
    for shift in range(shares):
        share = lax.rem(share_ref[0] + shift, shares)
        refs[shift][...] = total_ref[:, pl.ds(share, 1)][:, 0].astype(BF)


def join_kernel(shares, part, *refs):
    out_ref = refs[-1]
    ka_ref, kp_ref, rp_ref, gain_ref = refs[:4]
    total = ka_ref[...].astype(F32)
    for ref in refs[4:-2]:
        total = total + ref[...].astype(F32)
    groups = total.shape[0]
    top = out_ref.shape[1] - kp_ref.shape[1]
    gain = gain_ref[...] * (1.0 / groups)
    width = gain.shape[1]
    tail = [gain[:, :LANES], jnp.concatenate([gain[:, LANES:], jnp.zeros((1, 2 * LANES - width), F32)], axis=1)]
    tail = jnp.concatenate(tail + [jnp.zeros((top - part - 2, LANES), F32)], axis=0)
    for group in range(groups):
        for share in range(shares):
            piece = total[group, share * part : (share + 1) * part]
            out_ref[group * shares + share, :top, :] = jnp.concatenate([piece, tail], axis=0).astype(BF)
    out_ref[:, top:, :] = (kp_ref[...].astype(F32) + rp_ref[...].astype(F32)).astype(BF)


def sum_kernel(shares, part, top, got_ref, out_ref, gain_ref):
    peers = out_ref.shape[0]
    gain = None
    for share in range(shares):
        total = got_ref[share, :top, :].astype(F32)
        for peer in range(share + shares, peers, shares):
            total = total + got_ref[peer, :top, :].astype(F32)
        tail = total[part : part + 2]
        gain = tail if gain is None else gain + tail
        total = total[:part].astype(BF)
        for peer in range(peers):
            out_ref[peer, share * part : (share + 1) * part, :] = total
    width = gain_ref.shape[1]
    gain_ref[...] = jnp.concatenate([gain[:1], gain[1:2, : width - LANES]], axis=1)
    total = jnp.sum(got_ref[:, top:, :].astype(F32), axis=0).astype(BF)
    for peer in range(peers):
        out_ref[peer, shares * part :, :] = total


def unpack_kernel(shares, part, chunk_a, chunk_p, flip, head_ref, half_ref, gain_ref, att_ref, point_ref, *refs):
    left_ref, right_ref, wide_ref, sems = refs[-4:]
    targets = refs[-13:-7]
    gain_out, point_out, att_out = refs[-7:-4]
    width = left_ref.shape[0]
    rows_a = shares * part

    def read_a(index, offset, take):
        group, share = divmod(index, shares)

        def read(source, start, count):
            row = share * part + start
            return half_ref[group * shares + source, row : row + count, :].astype(F32)

        return get_rows(read, part, offset, take)

    def read_p(index, offset, take):
        return half_ref[index, rows_a + offset : rows_a + offset + take, :].astype(F32)

    for slot in range(wide_ref.shape[1] // LANES):
        wide_ref[:, slot * LANES : (slot + 1) * LANES] = get_rows(read_p, chunk_p, slot * width, width)
    left_ref[:, :LANES] = get_rows(read_a, chunk_a, 0, width)
    right_ref[:, :LANES] = get_rows(read_a, chunk_a, width, width)
    pair = get_rows(read_a, chunk_a, 2 * width, width)
    rest = width - LANES
    left_ref[:, LANES:] = pair[:, :rest]
    right_ref[:, LANES:] = pair[:, rest:]
    if not flip:
        extras = [
            pltpu.make_async_copy(gain_ref, gain_out, sems.at[3]),
            pltpu.make_async_copy(point_ref, point_out, sems.at[4]),
            pltpu.make_async_copy(att_ref, att_out, sems.at[5]),
        ]
        for extra in extras:
            extra.start()
    half = 1 - head_ref[0] if flip else head_ref[0]
    for which in range(2):

        @pl.when(half == which)
        def _():
            copies = [
                pltpu.make_async_copy(source, target, sems.at[place])
                for place, (source, target) in enumerate(
                    zip((left_ref, right_ref, wide_ref), targets[3 * which : 3 * which + 3])
                )
            ]
            for copy in copies:
                copy.start()
            for copy in copies:
                copy.wait()

    if not flip:
        for extra in extras:
            extra.wait()


def on_device(
    point_feats, block_anchor, anchor_feats, query_feats, out_grad, norm_gain,
    w_in, w_out, w_query, w_key, w_value, w_proj,
):
    team = ("geom", "head")
    crowd = ("geom", "design")
    owners = lax.axis_size(team)
    peers = lax.axis_size(crowd)
    xt = point_feats[0].T
    qt = query_feats[0].T
    gt = out_grad[0].T
    wot = w_out.T
    blocks = block_anchor.shape[1]
    per_owner, width = anchor_feats.shape[1:]
    points = xt.shape[1]
    queries = qt.shape[1]
    hid = w_in.shape[1]
    size = points // blocks
    anchors = owners * per_owner
    rows = round_up(max(per_owner, blocks + 2), 16)
    shares = lax.axis_size("design")
    head = lax.axis_index("head").astype(jnp.int32).reshape(1)
    share = lax.axis_index("design").astype(jnp.int32).reshape(1)
    pieces = 2 * peers
    chunk_a = 6 * width // pieces
    rows_a = round_up(chunk_a, 4 * shares)
    part = rows_a // shares
    top = round_up(part + 2, 8)
    chunk_p = 2 * width * hid // LANES // pieces

    send, hsum = call(
        functools.partial(pool_kernel, blocks),
        [((owners, rows, 2 * width), BF), ((round_up(blocks, 8), hid), F32)],
        xt, w_in, wot, anchor_feats[0], block_anchor,
    )
    got = lax.all_to_all(send, team, 0, 0, tiled=True)
    qp, dmix, wk, wv, gain_row, qn, gn, wpn, slope = call(
        functools.partial(query_kernel, blocks),
        [
            ((width, queries), BF),
            ((width, queries), BF),
            ((width, width), BF),
            ((width, width), BF),
            ((1, width), F32),
            ((width, queries), BF),
            ((width, queries), BF),
            ((width, width), BF),
            ((hid, points), BF),
        ],
        qt, gt, w_query, w_proj, w_key, w_value, norm_gain.reshape(1, width), xt, w_in,
    )
    pair_shape = (HEADS, anchors, queries)
    rows_out, normed, kv, probs, dscore, kvt = call(
        functools.partial(attend_kernel, blocks, size, per_owner),
        [
            ((owners, rows * width // LANES, LANES), BF),
            ((anchors, width), BF),
            ((anchors, 2 * width), BF),
            (pair_shape, BF),
            (pair_shape, BF),
            ((anchors, 2 * width), BF),
        ],
        *near(got, gain_row, wk, wv, qp, dmix),
    )
    back = lax.all_to_all(rows_out, team, 0, 0, tiled=True)
    shape_a = ((peers, rows_a, LANES), BF)
    mixed, keep_a, send_a = call(
        functools.partial(finish_kernel, chunk_a),
        [((width, queries), BF), shape_a, shape_a],
        head, *near(probs, dscore, kv, kvt, normed, qn, gn),
        scratch=[pltpu.VMEM((width, queries), BF), pltpu.VMEM((pieces, rows_a, LANES), BF)],
        smem=1,
    )
    both, win, attended = call(
        fetch_kernel,
        [((width, points + hid), BF), ((width, hid), BF), ((width, queries), BF)],
        *near(mixed, wpn),
        scratch=[pltpu.SemaphoreType.DMA((3,))],
        raw=(xt, wot, w_in) + near(send_a),
    )
    swap = [(0, 1), (1, 0)]
    shape_p = ((peers, chunk_p, LANES), BF)
    recv_a = lax.ppermute(send_a, "head", swap)
    groups = peers // shares
    shape_d = ((groups, rows_a, LANES), BF)
    keep_d, *sends_d = call(
        functools.partial(design_kernel, shares),
        [shape_d] * shares,
        share, *near(keep_a, recv_a),
        scratch=[pltpu.VMEM((groups, shares, rows_a, LANES), F32)],
        smem=1,
    )
    recvs_d = [
        lax.ppermute(send, "design", [(i, (i + shift) % shares) for i in range(shares)])
        for shift, send in enumerate(sends_d, 1)
    ]
    dpre, keep_p, send_p, dgain = call(
        functools.partial(back_kernel, blocks, chunk_p),
        [((hid, points), BF), shape_p, shape_p, ((1, width), F32)],
        head, *near(back, both, slope, hsum),
        scratch=[pltpu.VMEM((pieces, chunk_p, LANES), BF)],
        smem=1,
        raw=near(keep_d),
    )
    recv_p = lax.ppermute(send_p, "head", swap)
    (point_grad,) = call(
        point_grad_kernel, [((width, points), BF)], *near(win, dpre), raw=near(send_p)
    )
    (joined,) = call(
        functools.partial(join_kernel, shares, part),
        [((peers, top + chunk_p, LANES), BF)],
        *near(keep_d, keep_p, recv_p, dgain, *recvs_d), raw=near(point_grad),
    )
    scattered = lax.all_to_all(joined, crowd, 0, 0, tiled=True)
    summed, gain = call(
        functools.partial(sum_kernel, shares, part, top),
        [((peers, rows_a + chunk_p, LANES), BF), ((1, width), F32)],
        *near(scattered),
    )
    mine = lax.all_to_all(summed, crowd, 0, 0, tiled=True)
    other = lax.ppermute(mine, "head", swap)
    square, wide = ((width, width), F32), ((width, hid), F32)
    grads = ()
    for flip, half in ((False, mine), (True, other)):
        grads = call(
            functools.partial(unpack_kernel, shares, part, chunk_a, chunk_p, flip),
            [square, square, wide] * 2 + [((1, width), F32), ((width, points), BF), ((width, queries), BF)],
            head, *near(half, gain),
            scratch=[pltpu.VMEM(*square), pltpu.VMEM(*square), pltpu.VMEM(*wide)]
            + [pltpu.SemaphoreType.DMA((6,))],
            smem=1,
            raw=near(attended, point_grad) + tuple(grads),
            update=True,
        )
    gq, gk, gin, gv, gp, gout, gain, point_grad, attended = grads
    return (
        attended.T[None], point_grad.T[None], gin, gout.T, gq, gk, gv, gp, gain.reshape(width),
    )


def solution(mesh):
    split = P(("groups", "design"), ("geom", "head"), None)
    placed = (split, P(("groups", "design"), ("geom", "head")), split, split, split) + (P(),) * 7
    grads = (P("groups", None),) * 6 + (P("groups"),)

    return jax.shard_map(
        on_device, mesh=mesh, in_specs=placed, out_specs=(split, split) + grads, check_vma=False
    )
```
